32 devices in a mesh: path: 8 (over y, x, core), tm: 4 (over z).
Axes of the slice: x: 2, y: 2, z: 4, core: 2. Of those that a mesh axis runs over, the one named last changes fastest.
Arguments:
- increments: bfloat16 [8192, 32, 1000], P(('path', 'tm')), may hold values from -6 to 6
- level_table: int32 [4096], replicated, may hold values from 0 to 4, as said below
- time_table: int32 [4096], replicated, may hold values from 0 to 31, as said below
Outputs:
- value_est: float32 [32], P('tm')
- grad_est: float32 [32, 1000], P('tm')
The draws below stay inside these ranges and needn't reach their ends.
Inputs may be any that keep to these rules, and one draw needn't show every extreme that they name: `level_table`: never falls from one block to the next. `time_table`: split the 32 time points into as many runs of consecutive points as the tm axis has devices; the 128 consecutive entries of each device fall equally into every run.
All inputs are finite; a program needn't handle non-finite values.
Results may differ from the reference program's by a relative error of at most 0.0003.
The reference program's roundings to bfloat16 on the way count: a program that leaves them out, or rounds other values in their place, can miss the bound.
Values may be sent and summed in bfloat16 or wider, within the bound.
No kernel may reach another device: no remote copies, remote signals or barrier semaphores. Data moves between devices by JAX's collectives and lax.ppermute only.
A program may use at most 128 MiB of HBM per device.

```python
import jax
import jax.numpy as jnp
from jax import lax

D = 1000
K = 32
LEVELS = 5
BLOCK = 2
BLK_DEV = 128
BLOCKS = 4096
PATHS = 8192
N_PATH = 8
N_TM = 4


def draw_level_table(key, part):
    drawn = jax.random.randint(jax.random.fold_in(key, 11), (BLOCKS,), 0, LEVELS, dtype=jnp.int32)
    return jnp.sort(drawn)


def draw_time_table(key, part):
    devices = BLOCKS // BLK_DEV
    group_len = K // N_TM
    base = jnp.repeat(jnp.arange(N_TM, dtype=jnp.int32), BLK_DEV // N_TM)
    dev_keys = jax.random.split(jax.random.fold_in(key, 23), devices)
    shuffled = jax.vmap(lambda one_key: jax.random.permutation(one_key, base))(dev_keys)
    inside = jax.random.randint(jax.random.fold_in(key, 37), (devices, BLK_DEV), 0, group_len, dtype=jnp.int32)
    return (shuffled * group_len + inside).reshape(BLOCKS)


def shard_levels(stream_key, shape, pieces, smallest, top_value):
    loudness, own = 1.0, jax.random.fold_in(stream_key, 6)
    for dim, shards_of in pieces:
        steps = jnp.exp(jax.random.uniform(jax.random.fold_in(own, dim), (shards_of,), jnp.float32, smallest / len(pieces), top_value / len(pieces)))
        loudness = loudness * jnp.repeat(steps, shape[dim] // shards_of).reshape([-1 if axis == dim else 1 for axis in range(len(shape))])
    return loudness


def normal_values(rng, dims, scale, most, shards=(), kind=jnp.bfloat16):
    gain = shard_levels(rng, dims, shards, -0.22, 0.18) if shards else 1.0
    values = jax.random.normal(rng, dims, jnp.float32) * scale * gain
    return jnp.minimum(jnp.maximum(values, -most), most).astype(kind)


def setup_inputs(seed: int = 0) -> dict:
    arg_keys = jax.random.split(jax.random.key(seed), 4)
    increments = normal_values(arg_keys[0], (PATHS, K, D), 1.0, 6.0, ((0, 32),))
    level_table = draw_level_table(jax.random.fold_in(arg_keys[3], 71), 0)
    time_table = draw_time_table(jax.random.fold_in(arg_keys[3], 71), 0)
    return dict(increments=increments, level_table=level_table, time_table=time_table)


horizon = 0.3

def stride_weights(levels, starts, steps_k, step_len):
    steps = jnp.arange(steps_k).astype(jnp.int32)
    fine_stride = jnp.power(2, LEVELS - 1 - levels).astype(jnp.int32)
    coarse = fine_stride * 2
    live_steps = steps[None, :] >= starts[:, None]
    on_fine = steps[None, :] % fine_stride[:, None] == 0
    on_coarse = (steps[None, :] % coarse[:, None] == 0) & (levels[:, None] > 0)
    term = fine_stride[:, None] * on_fine.astype(jnp.int32) - coarse[:, None] * on_coarse.astype(jnp.int32)
    return step_len * (live_steps.astype(jnp.float32) * term.astype(jnp.float32))

def terminal(incr, starts):
    steps_k = incr.shape[1]
    width = incr.shape[2]
    step_len = horizon / steps_k
    steps = jnp.arange(steps_k).astype(jnp.int32)
    live_steps = (steps[None, :] >= starts[:, None]).astype(jnp.float32)
    end_point = jnp.sqrt(step_len) * jnp.einsum('pi,pid->pd', live_steps, incr.astype(jnp.float32), precision=lax.Precision.HIGHEST)
    remaining = horizon - starts.astype(jnp.float32) * step_len
    scaled = end_point / remaining[:, None]
    end_value = 1.0 / (2.0 + 0.4 * lax.optimization_barrier(jnp.sum(end_point * end_point, axis=1)) / width)
    return (scaled, end_value)

def partial_sums(path_total, scaled, row_index, path_share, row_count):
    select = (row_index[:, None] == jnp.arange(row_count).astype(jnp.int32)[None, :]).astype(jnp.float32)
    select = select * (path_share * path_total)[:, None]
    return (lax.optimization_barrier(jnp.sum(select, axis=0)), jnp.dot(select.T, scaled, precision=lax.Precision.HIGHEST))

def first_terms(incr, levels, starts, path_share, row_count, offset):
    scaled, end_value = terminal(incr, starts)
    path_total = end_value * (levels == 0).astype(jnp.float32)
    return partial_sums(path_total, scaled, starts - offset, path_share, row_count)

def second_terms(incr, levels, starts, path_share, value_one, grad_low, row_count, offset):
    paths, steps_k, width = incr.shape
    step_len = horizon / steps_k
    scaled, end_value = terminal(incr, starts)
    inner_dots = jnp.dot(incr.reshape(paths * steps_k, width), grad_low.T, preferred_element_type=jnp.float32).reshape(paths, steps_k, steps_k)
    steps = jnp.arange(steps_k).astype(jnp.int32)
    window = (steps[None, :, None] >= starts[:, None, None]) & (steps[None, :, None] < steps[None, None, :])
    estimate = value_one[None, :] + jnp.sqrt(step_len) * lax.optimization_barrier(jnp.sum(inner_dots * window.astype(jnp.float32), axis=1))
    drift_term = estimate - estimate * estimate * estimate
    weights = stride_weights(levels, starts, steps_k, step_len)
    path_total = end_value * (levels == 0).astype(jnp.float32) + lax.optimization_barrier(jnp.sum(weights * drift_term, axis=1))
    return partial_sums(path_total, scaled, starts - offset, path_share, row_count)

def reference(increments, level_table, time_table):
    steps_k = increments.shape[1]
    width = increments.shape[2]
    devices = N_PATH * N_TM
    lvl_hot = (level_table[:, None] == jnp.arange(LEVELS).astype(jnp.int32)[None, :]).astype(jnp.float32)
    time_hot = (time_table[:, None] == jnp.arange(steps_k).astype(jnp.int32)[None, :]).astype(jnp.float32)
    counts = jnp.dot(lvl_hot.T, time_hot, precision=lax.Precision.HIGHEST)
    lvl_path = jnp.repeat(level_table, BLOCK)
    time_path = jnp.repeat(time_table, BLOCK)
    path_share = 1.0 / (BLOCK * counts[lvl_path, time_path])
    inc_groups = increments.reshape(devices, -1, steps_k, width)
    lvl_groups = lvl_path.reshape(devices, -1)
    time_groups = time_path.reshape(devices, -1)
    share_groups = path_share.reshape(devices, -1)
    first_v, first_z = lax.map(lambda item: first_terms(item[0], item[1], item[2], item[3], steps_k, 0), (inc_groups, lvl_groups, time_groups, share_groups))
    value_one = lax.optimization_barrier(jnp.sum(first_v, axis=0))
    grad_one = lax.optimization_barrier(jnp.sum(first_z, axis=0))
    grad_low = grad_one.astype(jnp.bfloat16)
    second_v, second_z = lax.map(lambda item: second_terms(item[0], item[1], item[2], item[3], value_one, grad_low, steps_k, 0), (inc_groups, lvl_groups, time_groups, share_groups))
    return (lax.optimization_barrier(jnp.sum(second_v, axis=0)), lax.optimization_barrier(jnp.sum(second_z, axis=0)))
```

```python
import functools

import jax
import jax.numpy as jnp
from jax import lax
from jax.experimental import pallas as pl
from jax.experimental.pallas import tpu as pltpu
from jax.sharding import PartitionSpec as P

LEVELS = 5
BLOCK = 2
LANES = 128

horizon = 0.3
f32, bf16, i32 = jnp.float32, jnp.bfloat16, jnp.int32


def round_up(value, unit):
    return -(-value // unit) * unit


def chunk_rows(width):
    return next(r for r in (40, 32, 48, 24, 16, 8) if width % r == 0)


def split3(x):
    hi = x.astype(bf16)
    rest = x - hi.astype(f32)
    mid = rest.astype(bf16)
    low = (rest - mid.astype(f32)).astype(bf16)
    return hi, mid, low


def split2(x):
    hi = x.astype(bf16)
    return hi, (x - hi.astype(f32)).astype(bf16)


def contract_last(a, b):
    return lax.dot_general(a, b, (((1,), (1,)), ((), ())), preferred_element_type=f32)


def dot(a, b):
    return jnp.dot(a, b, preferred_element_type=f32)


def path_rows(lvl_ref, time_ref, steps_k, blk_dev, my_block):
    paths = BLOCK * blk_dev
    blocks = lvl_ref.shape[1]
    start = pl.multiple_of(my_block, LANES)
    own = jnp.concatenate(
        [lvl_ref[:, pl.ds(start, blk_dev)], time_ref[:, pl.ds(start, blk_dev)]], axis=0
    ).astype(f32)
    own = jnp.concatenate([own, jnp.zeros((6, blk_dev), f32)], axis=0).astype(bf16)
    block_of = lax.broadcasted_iota(i32, (blk_dev, paths), 1) // BLOCK
    repeat = (block_of == lax.broadcasted_iota(i32, (blk_dev, paths), 0)).astype(f32).astype(bf16)
    both = dot(own, repeat)
    level, start_t = both[0:1], both[1:2]
    lvl_hot = (lax.broadcasted_iota(i32, (8, blocks), 0) == lvl_ref[...]).astype(f32).astype(bf16)
    time_hot = (
        (lax.broadcasted_iota(i32, (steps_k, blocks), 0) == time_ref[...]).astype(f32).astype(bf16)
    )
    counts = contract_last(lvl_hot, time_hot)
    high = jnp.floor(counts * (1.0 / 256.0))
    low = counts - 256.0 * high
    own_time = start_hot(start_t, steps_k)
    at_time = 256.0 * dot(high.astype(bf16), own_time) + dot(low.astype(bf16), own_time)
    own_lvl = lax.broadcasted_iota(i32, (8, paths), 0).astype(f32) == level
    count = jnp.sum(jnp.where(own_lvl, at_time, 0.0), axis=0, keepdims=True)
    return level, start_t, 1.0 / (BLOCK * count)


def start_hot(start_t, steps_k):
    rows = lax.broadcasted_iota(i32, (steps_k, start_t.shape[1]), 0).astype(f32)
    return (rows == start_t).astype(f32).astype(bf16)


def weighted_sums(end_ref, store, hot, coef, value_row, width, split):
    full = end_ref.shape[0]
    for c in range(full // LANES):
        y = end_ref[c * LANES : (c + 1) * LANES, :] * coef
        if c * LANES <= width < (c + 1) * LANES:
            row = lax.broadcasted_iota(i32, y.shape, 0)
            y = jnp.where(row == width - c * LANES, value_row, y)
        store(c, sum(contract_last(hot, part) for part in split(y)))


def first_kernel(
    n_path, n_tm, inc_ref, lvl_ref, time_ref, out_ref, end_ref, rows_ref, buf, sems
):
    steps_k, width, paths = inc_ref.shape
    blk_dev = paths // BLOCK
    step_len = horizon / steps_k
    rows = chunk_rows(width)
    chunks = width // rows

    def copy(c):
        part = pl.ds(pl.multiple_of(c * rows, 8), rows)
        return pltpu.make_async_copy(inc_ref.at[:, part, :], buf.at[:, part, :], sems.at[c])

    @pl.loop(0, chunks)
    def _(c):
        copy(c).start()

    me = lax.axis_index("path") * n_tm + lax.axis_index("tm")
    level, start_t, share = path_rows(lvl_ref, time_ref, steps_k, blk_dev, me * blk_dev)
    tile_start = jnp.broadcast_to(start_t, (8, paths))

    def chunk(c, norm):
        copy(c).wait()
        base = pl.multiple_of(c * rows, 8)
        acc = [jnp.zeros((8, paths), f32) for _ in range(rows // 8)]
        for i in range(steps_k):
            live = tile_start <= float(i)
            x = buf[i, pl.ds(base, rows), :].astype(f32)
            for r in range(rows // 8):
                acc[r] = acc[r] + jnp.where(live, x[8 * r : 8 * r + 8], 0.0)
        root = jnp.sqrt(jnp.float32(step_len))
        for r in range(rows // 8):
            end = root * acc[r]
            end_ref[pl.ds(pl.multiple_of(base + 8 * r, 8), 8), :] = end
            norm = norm + end * end
        return norm

    norm = lax.fori_loop(0, chunks, chunk, jnp.zeros((8, paths), f32))
    full = end_ref.shape[0]
    end_ref[width:full, :] = jnp.zeros((full - width, paths), f32)
    value = 1.0 / (2.0 + 0.4 * jnp.sum(norm, axis=0, keepdims=True) / width)
    first = jnp.where(level == 0.0, value, 0.0)
    remaining = horizon - start_t * step_len
    coef = share / remaining
    hot = start_hot(start_t, steps_k)
    rows_ref[...] = jnp.concatenate(
        [level, start_t, first, share, coef, jnp.zeros((3, paths), f32)], axis=0
    )
    group, cols = out_ref.shape[2], out_ref.shape[3]

    def store(c, tile):
        for part in range(LANES // cols):
            a = c * (LANES // cols) + part
            for b in range(n_tm):
                out_ref[a, b] = tile[group * b : group * (b + 1), cols * part : cols * (part + 1)]

    weighted_sums(end_ref, store, hot, coef * first, share * first, width, split3)


def second_kernel(n_path, n_tm, inc_ref, z_ref, end_ref, rows_ref, out_ref, buf, z_all, sems):
    steps_k, width, paths = inc_ref.shape
    step_len = horizon / steps_k

    def copy(i):
        return pltpu.make_async_copy(inc_ref.at[i], buf.at[i], sems.at[i])

    @pl.loop(0, steps_k)
    def _(i):
        copy(i).start()

    group, cols = z_ref.shape[2], z_ref.shape[3]
    for a in range(n_path):
        for b in range(n_tm):
            z_all[group * b : group * (b + 1), cols * a : cols * (a + 1)] = z_ref[a, b]
    value_one = z_all[:, width : width + 1]
    z_low = z_all[:, 0:width].astype(bf16)
    level, start_t, first, share, coef = (rows_ref[r : r + 1, :] for r in range(5))
    at = lax.broadcasted_iota(i32, (steps_k, paths), 0)

    total = jnp.zeros((steps_k, paths), f32)
    for i in range(steps_k - 1):
        copy(i).wait()
        dots = dot(z_low, buf[i])
        seen = (at > i) & (start_t <= float(i))
        total = total + jnp.where(seen, dots, 0.0)
    copy(steps_k - 1).wait()
    estimate = value_one + jnp.sqrt(jnp.float32(step_len)) * total
    drift = estimate - estimate * estimate * estimate
    lvl = level.astype(i32)
    fine = lax.shift_left(jnp.ones_like(lvl), LEVELS - 1 - lvl)
    on_fine = (at & (fine - 1)) == 0
    on_coarse = ((at & (2 * fine - 1)) == 0) & (lvl > 0)
    weight = jnp.where(on_fine, fine, 0) - jnp.where(on_coarse, 2 * fine, 0)
    weight = jnp.where(at.astype(f32) >= start_t, weight.astype(f32), 0.0) * step_len
    second = first + jnp.sum(weight * drift, axis=0, keepdims=True)
    hot = start_hot(start_t, steps_k)

    def store(c, tile):
        for b in range(n_tm):
            out_ref[b, :, c * LANES : (c + 1) * LANES] = tile[group * b : group * (b + 1)]

    weighted_sums(end_ref, store, hot, coef * second, share * second, width, split2)


def params():
    return pltpu.CompilerParams(vmem_limit_bytes=48 * 1024 * 1024)


def shards(n_path, n_tm, increments, level_table, time_table):
    paths, steps_k, width = increments.shape
    group = steps_k // n_tm
    full = round_up(width + 1, LANES * max(1, n_path // LANES))
    cols = full // n_path
    inc = jnp.transpose(increments, (1, 2, 0))
    vmem = pl.BlockSpec(memory_space=pltpu.VMEM)
    hbm = pl.BlockSpec(memory_space=pl.ANY)
    chunks = width // chunk_rows(width)

    pieces, end, rows = pl.pallas_call(
        functools.partial(first_kernel, n_path, n_tm),
        out_shape=(
            jax.ShapeDtypeStruct((n_path, n_tm, group, cols), f32),
            jax.ShapeDtypeStruct((full, paths), f32),
            jax.ShapeDtypeStruct((8, paths), f32),
        ),
        in_specs=[hbm, vmem, vmem],
        out_specs=(vmem, vmem, vmem),
        scratch_shapes=[
            pltpu.VMEM((steps_k, width, paths), bf16),
            pltpu.SemaphoreType.DMA((chunks,)),
        ],
        compiler_params=params(),
        name="first_iterate",
    )(inc, level_table.reshape(1, -1), time_table.reshape(1, -1))

    def exchange(x):
        return lax.all_to_all(x, ("path", "tm"), 0, 0, tiled=True)

    received = exchange(pieces.reshape(n_path * n_tm, group, cols))
    own = jnp.sum(received, axis=0)
    spread = exchange(jnp.broadcast_to(own[None], received.shape))

    parts = pl.pallas_call(
        functools.partial(second_kernel, n_path, n_tm),
        out_shape=jax.ShapeDtypeStruct((n_tm, group, full), f32),
        in_specs=[hbm, vmem, vmem, vmem],
        out_specs=vmem,
        scratch_shapes=[
            pltpu.VMEM((steps_k, width, paths), bf16),
            pltpu.VMEM((steps_k, full), f32),
            pltpu.SemaphoreType.DMA((steps_k,)),
        ],
        compiler_params=params(),
        name="second_iterate",
    )(inc, spread.reshape(n_path, n_tm, group, cols), end, rows)

    over_tm = jnp.sum(lax.all_to_all(parts, "tm", 0, 0, tiled=True), axis=0)
    total = jnp.sum(lax.all_gather(over_tm, "path"), axis=0)
    return total[:, width], total[:, :width]


def solution(mesh):
    placed = (P(("path", "tm"), None, None), P(), P())
    return jax.shard_map(
        functools.partial(shards, mesh.shape["path"], mesh.shape["tm"]),
        mesh=mesh,
        in_specs=placed,
        out_specs=(P("tm"), P("tm", None)),
        check_vma=False,
    )
```

```python
import functools

import jax
import jax.numpy as jnp
from jax import lax
from jax.experimental import pallas as pl
from jax.experimental.pallas import tpu as pltpu
from jax.sharding import PartitionSpec as P

LEVELS = 5
BLOCK = 2
LANES = 128
VALUE_COPIES = 3
VMEM_LIMIT = 24 * 1024 * 1024

horizon = 0.3
f32, bf16, i32 = jnp.float32, jnp.bfloat16, jnp.int32


def round_up(value, unit):
    return -(-value // unit) * unit


def chunk_rows(width):
    return next(r for r in (40, 32, 48, 24, 16, 8) if width % r == 0)


def split3(x):
    hi = x.astype(bf16)
    rest = x - hi.astype(f32)
    mid = rest.astype(bf16)
    low = (rest - mid.astype(f32)).astype(bf16)
    return hi, mid, low


def split2(x):
    hi = x.astype(bf16)
    return hi, (x - hi.astype(f32)).astype(bf16)


def contract_last(a, b):
    return lax.dot_general(a, b, (((1,), (1,)), ((), ())), preferred_element_type=f32)


def dot(a, b):
    return jnp.dot(a, b, preferred_element_type=f32)


def path_rows(lvl_ref, time_ref, steps_k, blk_dev, my_block):
    paths = BLOCK * blk_dev
    blocks = lvl_ref.shape[1]
    start = pl.multiple_of(my_block, LANES)
    own = jnp.concatenate(
        [lvl_ref[:, pl.ds(start, blk_dev)], time_ref[:, pl.ds(start, blk_dev)]], axis=0
    ).astype(f32)
    own = jnp.concatenate([own, jnp.zeros((6, blk_dev), f32)], axis=0).astype(bf16)
    block_of = lax.broadcasted_iota(i32, (blk_dev, paths), 1) // BLOCK
    repeat = (block_of == lax.broadcasted_iota(i32, (blk_dev, paths), 0)).astype(f32).astype(bf16)
    both = dot(own, repeat)
    level, start_t = both[0:1], both[1:2]
    lvl_hot = (lax.broadcasted_iota(i32, (8, blocks), 0) == lvl_ref[...]).astype(f32).astype(bf16)
    time_hot = (
        (lax.broadcasted_iota(i32, (steps_k, blocks), 0) == time_ref[...]).astype(f32).astype(bf16)
    )
    counts = contract_last(lvl_hot, time_hot)
    high = jnp.floor(counts * (1.0 / 256.0))
    low = counts - 256.0 * high
    own_time = start_hot(start_t, steps_k)
    at_time = 256.0 * dot(high.astype(bf16), own_time) + dot(low.astype(bf16), own_time)
    own_lvl = lax.broadcasted_iota(i32, (8, paths), 0).astype(f32) == level
    count = jnp.sum(jnp.where(own_lvl, at_time, 0.0), axis=0, keepdims=True)
    return level, start_t, 1.0 / (BLOCK * count)


def start_hot(start_t, steps_k):
    rows = lax.broadcasted_iota(i32, (steps_k, start_t.shape[1]), 0).astype(f32)
    return (rows == start_t).astype(f32).astype(bf16)


def weighted_sums(end_ref, store, hot, coef, value_row, width, split):
    full = end_ref.shape[0]
    for c in range(full // LANES):
        y = end_ref[c * LANES : (c + 1) * LANES, :] * coef
        if (c + 1) * LANES > width:
            row = lax.broadcasted_iota(i32, y.shape, 0) + (c * LANES - width)
            y = jnp.where((row >= 0) & (row < VALUE_COPIES), value_row, y)
        store(c, sum(contract_last(hot, part) for part in split(y)))


def first_kernel(
    n_path, n_tm, inc_ref, lvl_hbm, time_hbm, mine_ref, other_ref, end_ref, rows_ref, buf,
    lvl_ref, time_ref, part_ref, sems, table_sems,
):
    steps_k, width, paths = inc_ref.shape
    blk_dev = paths // BLOCK
    step_len = horizon / steps_k
    rows = chunk_rows(width)
    chunks = width // rows

    def copy(c):
        part = pl.ds(pl.multiple_of(c * rows, 8), rows)
        return pltpu.make_async_copy(inc_ref.at[:, part, :], buf.at[:, part, :], sems.at[c])

    tables = [
        pltpu.make_async_copy(lvl_hbm, lvl_ref, table_sems.at[0]),
        pltpu.make_async_copy(time_hbm, time_ref, table_sems.at[1]),
    ]
    for table in tables:
        table.start()

    @pl.loop(0, chunks)
    def _(c):
        copy(c).start()

    for table in tables:
        table.wait()
    me = lax.axis_index("path") * n_tm + lax.axis_index("tm")
    level, start_t, share = path_rows(lvl_ref, time_ref, steps_k, blk_dev, me * blk_dev)
    tile_start = jnp.broadcast_to(start_t, (8, paths))

    def chunk(c, norm):
        copy(c).wait()
        base = pl.multiple_of(c * rows, 8)
        acc = [jnp.zeros((8, paths), f32) for _ in range(rows // 8)]
        for i in range(steps_k):
            live = tile_start <= float(i)
            x = buf[i, pl.ds(base, rows), :].astype(f32)
            for r in range(rows // 8):
                acc[r] = acc[r] + jnp.where(live, x[8 * r : 8 * r + 8], 0.0)
        root = jnp.sqrt(jnp.float32(step_len))
        for r in range(rows // 8):
            end = root * acc[r]
            end_ref[pl.ds(pl.multiple_of(base + 8 * r, 8), 8), :] = end
            norm = norm + end * end
        return norm

    norm = lax.fori_loop(0, chunks, chunk, jnp.zeros((8, paths), f32))
    full = end_ref.shape[0]
    end_ref[width:full, :] = jnp.zeros((full - width, paths), f32)
    value = 1.0 / (2.0 + 0.4 * jnp.sum(norm, axis=0, keepdims=True) / width)
    first = jnp.where(level == 0.0, value, 0.0)
    remaining = horizon - start_t * step_len
    coef = share / remaining
    hot = start_hot(start_t, steps_k)
    rows_ref[...] = jnp.concatenate(
        [level, start_t, first, share, coef, jnp.zeros((3, paths), f32)], axis=0
    )
    half = mine_ref.shape[1]

    def store(c, tile):
        side, at = divmod(c * LANES, half)
        part_ref[side, :, at : at + LANES] = tile

    weighted_sums(end_ref, store, hot, coef * first, share * first, width, split3)
    side = lax.axis_index("path") % 2
    mine_ref[...] = part_ref[side]
    other_ref[...] = part_ref[1 - side]


def second_kernel(
    n_path, n_tm, buf, mine_ref, other_ref, end_ref, rows_ref, out_mine, out_other, z_ref, part_ref
):
    steps_k, width, paths = buf.shape
    step_len = horizon / steps_k
    half = mine_ref.shape[1]
    group = steps_k // n_tm
    side = lax.axis_index("path") % 2
    z_ref[side] = mine_ref[...].astype(f32)
    z_ref[1 - side] = other_ref[...].astype(f32)
    value_one = sum(
        z_ref[1, :, width + r - half : width + r - half + 1] for r in range(VALUE_COPIES)
    )
    z_low = jnp.concatenate([z_ref[0], z_ref[1]], axis=1)[:, :width].astype(bf16)
    level, start_t, first, share, coef = (rows_ref[r : r + 1, :] for r in range(5))
    at = lax.broadcasted_iota(i32, (steps_k, paths), 0)

    total = jnp.zeros((steps_k, paths), f32)
    for i in range(steps_k - 1):
        dots = dot(z_low, buf[i])
        seen = (at > i) & (start_t <= float(i))
        total = total + jnp.where(seen, dots, 0.0)
    estimate = value_one + jnp.sqrt(jnp.float32(step_len)) * total
    drift = estimate - estimate * estimate * estimate
    lvl = level.astype(i32)
    fine = lax.shift_left(jnp.ones_like(lvl), LEVELS - 1 - lvl)
    on_fine = (at & (fine - 1)) == 0
    on_coarse = ((at & (2 * fine - 1)) == 0) & (lvl > 0)
    weight = jnp.where(on_fine, fine, 0) - jnp.where(on_coarse, 2 * fine, 0)
    weight = jnp.where(at.astype(f32) >= start_t, weight.astype(f32), 0.0) * step_len
    second = first + jnp.sum(weight * drift, axis=0, keepdims=True)
    hot = start_hot(start_t, steps_k)

    def store(c, tile):
        part, at = divmod(c * LANES, half)
        part_ref[part, :, at : at + LANES] = tile

    weighted_sums(end_ref, store, hot, coef * second, share * second, width, split2)
    me = lax.axis_index("tm")
    for away in range(n_tm):
        rows = pl.ds(pl.multiple_of((me ^ away) * group, group), group)
        out_mine[away] = part_ref[side, rows, :]
        out_other[away] = part_ref[1 - side, rows, :]


def params():
    return pltpu.CompilerParams(vmem_limit_bytes=VMEM_LIMIT)


def in_hbm(x):
    return pltpu.with_memory_space_constraint(x, pltpu.HBM)


def swap(x, axis, offset):
    return lax.ppermute(x, axis, [(i, i ^ offset) for i in range(lax.axis_size(axis))])


def add_kernel(*refs):
    *parts, out_ref = refs
    out_ref[...] = pairwise([part[...] for part in parts])


def round_kernel(width, *refs):
    *parts, out_ref = refs
    total = pairwise([part[...] for part in parts])
    first = lax.axis_index("path") % 2 * total.shape[1] - width
    column = lax.broadcasted_iota(i32, total.shape, 1) + first
    high, middle, low = (part.astype(f32) for part in split3(total))
    out_ref[...] = jnp.where(column == 1, middle, jnp.where(column == 2, low, high)).astype(bf16)


def pairwise(parts):
    while len(parts) > 1:
        parts = [a + b for a, b in zip(parts[::2], parts[1::2])]
    return parts[0]


def local(kernel, dtype, parts):
    vmem = pl.BlockSpec(memory_space=pltpu.VMEM)
    return pl.pallas_call(
        kernel,
        out_shape=jax.ShapeDtypeStruct(parts[0].shape, dtype),
        in_specs=[vmem] * len(parts),
        out_specs=vmem,
        compiler_params=pltpu.CompilerParams(vmem_limit_bytes=4 * 1024 * 1024),
    )(*parts)


def terms(x, axis, first_bit):
    ways = 4 if 2 * first_bit < lax.axis_size(axis) else 2
    return [x] + [swap(x, axis, first_bit * away) for away in range(1, ways)]


def steps_over(axis, first_bit):
    bits = []
    while first_bit < lax.axis_size(axis):
        bits.append((axis, first_bit))
        first_bit *= 4
    return bits


def shards(n_path, n_tm, increments, level_table, time_table):
    paths, steps_k, width = increments.shape
    group = steps_k // n_tm
    full = round_up(width + VALUE_COPIES, 2 * LANES)
    half = full // 2
    inc = jnp.transpose(increments, (1, 2, 0))
    vmem = pl.BlockSpec(memory_space=pltpu.VMEM)
    hbm = pl.BlockSpec(memory_space=pltpu.HBM)
    chunks = width // chunk_rows(width)
    side = lax.axis_index("path") % 2

    mine, other, end, rows, held = pl.pallas_call(
        functools.partial(first_kernel, n_path, n_tm),
        out_shape=(
            jax.ShapeDtypeStruct((steps_k, half), f32),
            jax.ShapeDtypeStruct((steps_k, half), f32),
            jax.ShapeDtypeStruct((full, paths), f32),
            jax.ShapeDtypeStruct((8, paths), f32),
            pltpu.VMEM(inc.shape, bf16),
        ),
        in_specs=[hbm, hbm, hbm],
        out_specs=(vmem,) * 5,
        scratch_shapes=[
            pltpu.VMEM((1, level_table.shape[0]), i32),
            pltpu.VMEM((1, time_table.shape[0]), i32),
            pltpu.VMEM((2, steps_k, half), f32),
            pltpu.SemaphoreType.DMA((chunks,)),
            pltpu.SemaphoreType.DMA((2,)),
        ],
        compiler_params=params(),
        name="first_iterate",
    )(inc, *(in_hbm(table.reshape(1, -1)) for table in (level_table, time_table)))

    parts = [mine, swap(other, "path", 1)]
    for step in steps_over("path", 2) + steps_over("tm", 1):
        parts = terms(local(add_kernel, f32, parts), *step)
    own = local(functools.partial(round_kernel, width), bf16, parts)

    mine, other = pl.pallas_call(
        functools.partial(second_kernel, n_path, n_tm),
        out_shape=(jax.ShapeDtypeStruct((n_tm, group, half), f32),) * 2,
        in_specs=[vmem] * 5,
        out_specs=(vmem, vmem),
        scratch_shapes=[pltpu.VMEM((2, steps_k, half), f32)] * 2,
        compiler_params=params(),
        name="second_iterate",
    )(pltpu.with_memory_space_constraint(held, pltpu.VMEM), own, swap(own, "path", 1), end, rows)

    part = mine + swap(other, "path", 1)
    own = pairwise([part[0]] + [swap(part[away], "tm", away) for away in range(1, n_tm)])
    for step in steps_over("path", 2):
        own = pairwise(terms(own, *step))
    other = swap(own, "path", 1)
    total = jnp.concatenate(
        [jnp.where(side == 0, own, other), jnp.where(side == 0, other, own)], axis=1
    )
    return total[:, width], total[:, :width]


def solution(mesh):
    placed = (P(("path", "tm"), None, None), P(), P())
    return jax.shard_map(
        functools.partial(shards, mesh.shape["path"], mesh.shape["tm"]),
        mesh=mesh,
        in_specs=placed,
        out_specs=(P("tm"), P("tm", None)),
        check_vma=False,
    )
```

```python
import functools

import jax
import jax.numpy as jnp
from jax import lax
from jax.experimental import pallas as pl
from jax.experimental.pallas import tpu as pltpu
from jax.sharding import PartitionSpec as P

LEVELS = 5
BLOCK = 2
LANES = 128
VALUE_COPIES = 3
PACKED = 16
VMEM_LIMIT = 24 * 1024 * 1024
SMALL_LIMIT = 4 * 1024 * 1024

horizon = 0.3
f32, bf16, i32 = jnp.float32, jnp.bfloat16, jnp.int32


def round_up(value, unit):
    return -(-value // unit) * unit


def chunk_rows(width):
    return next(r for r in (40, 32, 48, 24, 16, 8) if width % r == 0)


def split3(x):
    hi = x.astype(bf16)
    rest = x - hi.astype(f32)
    mid = rest.astype(bf16)
    low = (rest - mid.astype(f32)).astype(bf16)
    return hi, mid, low


def split2(x):
    hi = x.astype(bf16)
    return hi, (x - hi.astype(f32)).astype(bf16)


def contract_last(a, b):
    return lax.dot_general(a, b, (((1,), (1,)), ((), ())), preferred_element_type=f32)


def dot(a, b):
    return jnp.dot(a, b, preferred_element_type=f32)


def path_rows(lvl_ref, time_ref, steps_k, blk_dev, my_block):
    paths = BLOCK * blk_dev
    blocks = lvl_ref.shape[1]
    start = pl.multiple_of(my_block, LANES)
    own = jnp.concatenate(
        [lvl_ref[:, pl.ds(start, blk_dev)], time_ref[:, pl.ds(start, blk_dev)]], axis=0
    ).astype(f32)
    own = jnp.concatenate([own, jnp.zeros((6, blk_dev), f32)], axis=0).astype(bf16)
    block_of = lax.broadcasted_iota(i32, (blk_dev, paths), 1) // BLOCK
    repeat = (block_of == lax.broadcasted_iota(i32, (blk_dev, paths), 0)).astype(f32).astype(bf16)
    both = dot(own, repeat)
    level, start_t = both[0:1], both[1:2]
    lvl_hot = (lax.broadcasted_iota(i32, (8, blocks), 0) == lvl_ref[...]).astype(f32).astype(bf16)
    time_hot = (
        (lax.broadcasted_iota(i32, (steps_k, blocks), 0) == time_ref[...]).astype(f32).astype(bf16)
    )
    counts = contract_last(lvl_hot, time_hot)
    high = jnp.floor(counts * (1.0 / 256.0))
    low = counts - 256.0 * high
    own_time = start_hot(start_t, steps_k)
    at_time = 256.0 * dot(high.astype(bf16), own_time) + dot(low.astype(bf16), own_time)
    own_lvl = lax.broadcasted_iota(i32, (8, paths), 0).astype(f32) == level
    count = jnp.sum(jnp.where(own_lvl, at_time, 0.0), axis=0, keepdims=True)
    return level, start_t, 1.0 / (BLOCK * count)


def start_hot(start_t, steps_k):
    rows = lax.broadcasted_iota(i32, (steps_k, start_t.shape[1]), 0).astype(f32)
    return (rows == start_t).astype(f32).astype(bf16)


def weighted_sums(end_ref, store, hot, coef, value_row, width, split):
    full = end_ref.shape[0]
    for c in range(full // LANES):
        y = end_ref[c * LANES : (c + 1) * LANES, :] * coef
        if (c + 1) * LANES > width:
            row = lax.broadcasted_iota(i32, y.shape, 0) + (c * LANES - width)
            y = jnp.where((row >= 0) & (row < VALUE_COPIES), value_row, y)
        store(c, sum(contract_last(hot, part) for part in split(y)))


def first_kernel(
    n_path, n_tm, inc_ref, lvl_hbm, time_hbm, mine_ref, other_ref, end_ref, rows_ref, buf,
    lvl_ref, time_ref, part_ref, mask_ref, sems, table_sems,
):
    steps_k, width, paths = inc_ref.shape
    blk_dev = paths // BLOCK
    step_len = horizon / steps_k
    rows = chunk_rows(width)
    chunks = width // rows

    def copy(c):
        part = pl.ds(pl.multiple_of(c * rows, 8), rows)
        return pltpu.make_async_copy(inc_ref.at[:, part, :], buf.at[:, part, :], sems.at[c])

    tables = [
        pltpu.make_async_copy(lvl_hbm, lvl_ref, table_sems.at[0]),
        pltpu.make_async_copy(time_hbm, time_ref, table_sems.at[1]),
    ]
    for table in tables:
        table.start()

    @pl.loop(0, chunks)
    def _(c):
        copy(c).start()

    for table in tables:
        table.wait()
    me = lax.axis_index("path") * n_tm + lax.axis_index("tm")
    level, start_t, share = path_rows(lvl_ref, time_ref, steps_k, blk_dev, me * blk_dev)
    tile_start = jnp.broadcast_to(start_t, (PACKED, paths))
    for i in range(steps_k):
        mask_ref[i] = (tile_start <= float(i)).astype(f32).astype(bf16)

    def chunk(c, norm):
        copy(c).wait()
        base = pl.multiple_of(c * rows, 8)
        acc = [jnp.zeros((8, paths), f32) for _ in range(rows // 8)]
        for i in range(steps_k):
            live = mask_ref[i]
            x = buf[i, pl.ds(base, rows), :]
            x = jnp.concatenate(
                [x[r : r + PACKED] * live[: min(PACKED, rows - r)] for r in range(0, rows, PACKED)],
                axis=0,
            )
            buf[i, pl.ds(base, rows), :] = x
            x = x.astype(f32)
            for r in range(rows // 8):
                acc[r] = acc[r] + x[8 * r : 8 * r + 8]
        root = jnp.sqrt(jnp.float32(step_len))
        for r in range(rows // 8):
            end = root * acc[r]
            end_ref[pl.ds(pl.multiple_of(base + 8 * r, 8), 8), :] = end
            norm = norm + end * end
        return norm

    norm = lax.fori_loop(0, chunks, chunk, jnp.zeros((8, paths), f32))
    full = end_ref.shape[0]
    end_ref[width:full, :] = jnp.zeros((full - width, paths), f32)
    value = 1.0 / (2.0 + 0.4 * jnp.sum(norm, axis=0, keepdims=True) / width)
    first = jnp.where(level == 0.0, value, 0.0)
    remaining = horizon - start_t * step_len
    coef = share / remaining
    hot = start_hot(start_t, steps_k)
    rows_ref[...] = jnp.concatenate(
        [level, start_t, first, share, coef, jnp.zeros((3, paths), f32)], axis=0
    )
    half = mine_ref.shape[1]

    def store(c, tile):
        side, at = divmod(c * LANES, half)
        part_ref[side, :, at : at + LANES] = tile

    weighted_sums(end_ref, store, hot, coef * first, share * first, width, split3)
    side = my_side()
    mine_ref[...] = part_ref[side]
    other_ref[...] = part_ref[1 - side]


def second_kernel(
    n_tm, buf, mine_ref, other_ref, end_ref, rows_ref, *refs
):
    *out_refs, z_ref, part_ref = refs
    steps_k, width, paths = buf.shape
    step_len = horizon / steps_k
    half = mine_ref.shape[1]
    group = steps_k // n_tm
    side = my_side()
    z_ref[side] = mine_ref[...].astype(f32)
    z_ref[1 - side] = other_ref[...].astype(f32)
    value_one = sum(
        z_ref[1, :, width + r - half : width + r - half + 1] for r in range(VALUE_COPIES)
    )
    z_low = jnp.concatenate([z_ref[0], z_ref[1]], axis=1).astype(bf16)
    z_cols = [z_low[:, c : c + LANES] for c in range(0, round_up(width, LANES), LANES)]
    level, start_t, first, share, coef = (rows_ref[r : r + 1, :] for r in range(5))
    at = lax.broadcasted_iota(i32, (steps_k, paths), 0)

    later = lax.broadcasted_iota(i32, (steps_k, LANES), 0)
    total = jnp.zeros((steps_k, paths), f32)
    for i in range(steps_k - 1):
        open_rows = (later > i).astype(f32).astype(bf16)
        z_open = jnp.concatenate([z * open_rows for z in z_cols], axis=1)[:, :width]
        total = total + dot(z_open, buf[i])
    estimate = value_one + jnp.sqrt(jnp.float32(step_len)) * total
    drift = estimate - estimate * estimate * estimate
    lvl = level.astype(i32)
    fine = lax.shift_left(jnp.ones_like(lvl), LEVELS - 1 - lvl)
    on_fine = (at & (fine - 1)) == 0
    on_coarse = ((at & (2 * fine - 1)) == 0) & (lvl > 0)
    weight = jnp.where(on_fine, fine, 0) - jnp.where(on_coarse, 2 * fine, 0)
    weight = jnp.where(at.astype(f32) >= start_t, weight.astype(f32), 0.0) * step_len
    second = first + jnp.sum(weight * drift, axis=0, keepdims=True)
    hot = start_hot(start_t, steps_k)

    def store(c, tile):
        part_ref[:, c * LANES : (c + 1) * LANES] = tile

    weighted_sums(end_ref, store, hot, coef * second, share * second, width, split2)
    me = lax.axis_index("tm")
    for away, out_ref in enumerate(out_refs):
        out_ref[...] = part_ref[pl.ds(pl.multiple_of((me ^ away) * group, group), group), :]


def last_kernel(width, *refs):
    *parts, value_ref, grad_ref, value_buf, grad_buf, sems = refs
    total = pairwise([part[...] for part in parts])
    group = total.shape[0]
    grad_buf[...] = total[:, :width]
    square = (group, group)
    eye = lax.broadcasted_iota(i32, square, 0) == lax.broadcasted_iota(i32, square, 1)
    column = jnp.broadcast_to(total[:, width : width + 1], square)
    value_buf[...] = jnp.sum(jnp.where(eye, column, 0.0), axis=0, keepdims=True)
    copies = [
        pltpu.make_async_copy(grad_buf, grad_ref, sems.at[0]),
        pltpu.make_async_copy(value_buf, value_ref, sems.at[1]),
    ]
    for copy in copies:
        copy.start()
    for copy in copies:
        copy.wait()


def params():
    return pltpu.CompilerParams(vmem_limit_bytes=VMEM_LIMIT)


def in_hbm(x):
    return pltpu.with_memory_space_constraint(x, pltpu.HBM)


def swap(x, path_xor, tm_xor):
    flip = path_xor * lax.axis_size("tm") + tm_xor
    devices = lax.axis_size(("path", "tm"))
    return lax.ppermute(x, ("path", "tm"), [(i, i ^ flip) for i in range(devices)])


def my_side():
    return lax.axis_index("path") & 1


def add_kernel(*refs):
    *parts, out_ref = refs
    out_ref[...] = pairwise([part[...] for part in parts])


def round_kernel(width, *refs):
    *parts, out_ref = refs
    total = pairwise([part[...] for part in parts])
    first = my_side() * total.shape[1] - width
    column = lax.broadcasted_iota(i32, total.shape, 1) + first
    high, middle, low = (part.astype(f32) for part in split3(total))
    out_ref[...] = jnp.where(column == 1, middle, jnp.where(column == 2, low, high)).astype(bf16)


def pairwise(parts):
    while len(parts) > 1:
        parts = [a + b for a, b in zip(parts[::2], parts[1::2])]
    return parts[0]


def local(kernel, dtype, parts):
    vmem = pl.BlockSpec(memory_space=pltpu.VMEM)
    return pl.pallas_call(
        kernel,
        out_shape=jax.ShapeDtypeStruct(parts[0].shape, dtype),
        in_specs=[vmem] * len(parts),
        out_specs=vmem,
        compiler_params=pltpu.CompilerParams(vmem_limit_bytes=SMALL_LIMIT),
    )(*parts)


def path_steps(n_path):
    steps, bit = [], 2
    while bit < n_path:
        steps.append((bit, 2 * bit, 3 * bit) if 2 * bit < n_path else (bit,))
        bit *= 4
    return steps


def tm_steps(n_tm):
    return [tuple(step // 2 for step in steps) for steps in path_steps(2 * n_tm)]


def shards(n_path, n_tm, increments, level_table, time_table):
    paths, steps_k, width = increments.shape
    group = steps_k // n_tm
    full = round_up(width + VALUE_COPIES, 2 * LANES)
    half = full // 2
    inc = jnp.transpose(increments, (1, 2, 0))
    vmem = pl.BlockSpec(memory_space=pltpu.VMEM)
    hbm = pl.BlockSpec(memory_space=pltpu.HBM)
    chunks = width // chunk_rows(width)

    mine, other, end, rows, held = pl.pallas_call(
        functools.partial(first_kernel, n_path, n_tm),
        out_shape=(
            jax.ShapeDtypeStruct((steps_k, half), f32),
            jax.ShapeDtypeStruct((steps_k, half), f32),
            jax.ShapeDtypeStruct((full, paths), f32),
            jax.ShapeDtypeStruct((8, paths), f32),
            jax.ShapeDtypeStruct(inc.shape, bf16),
        ),
        in_specs=[hbm, hbm, hbm],
        out_specs=(vmem,) * 5,
        scratch_shapes=[
            pltpu.VMEM((1, level_table.shape[0]), i32),
            pltpu.VMEM((1, time_table.shape[0]), i32),
            pltpu.VMEM((2, steps_k, half), f32),
            pltpu.VMEM((steps_k, PACKED, paths), bf16),
            pltpu.SemaphoreType.DMA((chunks,)),
            pltpu.SemaphoreType.DMA((2,)),
        ],
        compiler_params=params(),
        name="first_iterate",
    )(inc, *(in_hbm(table.reshape(1, -1)) for table in (level_table, time_table)))

    parts = [mine, swap(other, 1, 0)]
    hops = [[(flip, 0) for flip in step] for step in path_steps(n_path)]
    hops += [[(0, flip) for flip in step] for step in tm_steps(n_tm)]
    for step in hops:
        total = local(add_kernel, f32, parts)
        parts = [total] + [swap(total, *flips) for flips in step]
    own = local(functools.partial(round_kernel, width), bf16, parts)

    parts = pl.pallas_call(
        functools.partial(second_kernel, n_tm),
        out_shape=(jax.ShapeDtypeStruct((group, full), f32),) * n_tm,
        in_specs=[vmem] * 5,
        out_specs=(vmem,) * n_tm,
        scratch_shapes=[pltpu.VMEM((2, steps_k, half), f32), pltpu.VMEM((steps_k, full), f32)],
        compiler_params=params(),
        name="second_iterate",
    )(held, own, swap(own, 1, 0), end, rows)

    own = pairwise([parts[0]] + [swap(parts[away], 1, away) for away in range(1, n_tm)])
    parts = [own, swap(own, 1, 0)]
    for step in path_steps(n_path):
        total = pairwise(parts)
        parts = [total] + [swap(total, flip + 1, 0) for flip in step]
    value, grad = pl.pallas_call(
        functools.partial(last_kernel, width),
        out_shape=(
            jax.ShapeDtypeStruct((1, group), f32),
            jax.ShapeDtypeStruct((group, width), f32),
        ),
        in_specs=[vmem] * len(parts),
        out_specs=(hbm, hbm),
        scratch_shapes=[
            pltpu.VMEM((1, group), f32),
            pltpu.VMEM((group, width), f32),
            pltpu.SemaphoreType.DMA((2,)),
        ],
        compiler_params=pltpu.CompilerParams(vmem_limit_bytes=SMALL_LIMIT),
        name="last_sum",
    )(*parts)
    return value.reshape(group), grad


def solution(mesh):
    placed = (P(("path", "tm"), None, None), P(), P())
    return jax.shard_map(
        functools.partial(shards, mesh.shape["path"], mesh.shape["tm"]),
        mesh=mesh,
        in_specs=placed,
        out_specs=(P("tm"), P("tm", None)),
        check_vma=False,
    )
```

```python
import functools

import jax
import jax.numpy as jnp
from jax import lax
from jax.experimental import pallas as pl
from jax.experimental.pallas import tpu as pltpu
from jax.sharding import PartitionSpec as P

LEVELS = 5
BLOCK = 2
LANES = 128
VALUE_COPIES = 3
PACKED = 16
VMEM_LIMIT = 24 * 1024 * 1024
SMALL_LIMIT = 4 * 1024 * 1024

horizon = 0.3
f32, bf16, i32 = jnp.float32, jnp.bfloat16, jnp.int32


def round_up(value, unit):
    return -(-value // unit) * unit


def chunk_rows(width):
    return next(r for r in (40, 32, 48, 24, 16, 8) if width % r == 0)


def split3(x):
    hi = x.astype(bf16)
    rest = x - hi.astype(f32)
    mid = rest.astype(bf16)
    low = (rest - mid.astype(f32)).astype(bf16)
    return hi, mid, low


def split2(x):
    hi = x.astype(bf16)
    return hi, (x - hi.astype(f32)).astype(bf16)


def contract_last(a, b):
    return lax.dot_general(a, b, (((1,), (1,)), ((), ())), preferred_element_type=f32)


def dot(a, b):
    return jnp.dot(a, b, preferred_element_type=f32)


def path_rows(lvl_ref, time_ref, steps_k, blk_dev, my_block):
    paths = BLOCK * blk_dev
    blocks = lvl_ref.shape[1]
    start = pl.multiple_of(my_block, LANES)
    own = jnp.concatenate(
        [lvl_ref[:, pl.ds(start, blk_dev)], time_ref[:, pl.ds(start, blk_dev)]], axis=0
    ).astype(f32)
    own = jnp.concatenate([own, jnp.zeros((6, blk_dev), f32)], axis=0).astype(bf16)
    block_of = lax.broadcasted_iota(i32, (blk_dev, paths), 1) // BLOCK
    repeat = (block_of == lax.broadcasted_iota(i32, (blk_dev, paths), 0)).astype(f32).astype(bf16)
    both = dot(own, repeat)
    level, start_t = both[0:1], both[1:2]
    lvl_hot = (lax.broadcasted_iota(i32, (8, blocks), 0) == lvl_ref[...]).astype(f32).astype(bf16)
    time_hot = (
        (lax.broadcasted_iota(i32, (steps_k, blocks), 0) == time_ref[...]).astype(f32).astype(bf16)
    )
    counts = contract_last(lvl_hot, time_hot)
    high = jnp.floor(counts * (1.0 / 256.0))
    low = counts - 256.0 * high
    own_time = start_hot(start_t, steps_k)
    at_time = 256.0 * dot(high.astype(bf16), own_time) + dot(low.astype(bf16), own_time)
    own_lvl = lax.broadcasted_iota(i32, (8, paths), 0).astype(f32) == level
    count = jnp.sum(jnp.where(own_lvl, at_time, 0.0), axis=0, keepdims=True)
    return level, start_t, 1.0 / (BLOCK * count)


def start_hot(start_t, steps_k):
    rows = lax.broadcasted_iota(i32, (steps_k, start_t.shape[1]), 0).astype(f32)
    return (rows == start_t).astype(f32).astype(bf16)


def weighted_sums(end_ref, store, hot, coef, value_row, width, split):
    full = end_ref.shape[0]
    for c in range(full // LANES):
        y = end_ref[c * LANES : (c + 1) * LANES, :] * coef
        if (c + 1) * LANES > width:
            row = lax.broadcasted_iota(i32, y.shape, 0) + (c * LANES - width)
            y = jnp.where((row >= 0) & (row < VALUE_COPIES), value_row, y)
        store(c, sum(contract_last(hot, part) for part in split(y)))


def first_kernel(
    n_path, n_tm, inc_ref, lvl_hbm, time_hbm, mine_ref, other_ref, end_ref, rows_ref, buf,
    lvl_ref, time_ref, part_ref, mask_ref, sems, table_sems,
):
    steps_k, width, paths = inc_ref.shape
    blk_dev = paths // BLOCK
    step_len = horizon / steps_k
    rows = chunk_rows(width)
    chunks = width // rows

    def copy(c):
        part = pl.ds(pl.multiple_of(c * rows, 8), rows)
        return pltpu.make_async_copy(inc_ref.at[:, part, :], buf.at[:, part, :], sems.at[c])

    tables = [
        pltpu.make_async_copy(lvl_hbm, lvl_ref, table_sems.at[0]),
        pltpu.make_async_copy(time_hbm, time_ref, table_sems.at[1]),
    ]
    for table in tables:
        table.start()

    @pl.loop(0, chunks)
    def _(c):
        copy(c).start()

    for table in tables:
        table.wait()
    me = lax.axis_index("path") * n_tm + lax.axis_index("tm")
    level, start_t, share = path_rows(lvl_ref, time_ref, steps_k, blk_dev, me * blk_dev)
    tile_start = jnp.broadcast_to(start_t, (PACKED, paths))
    for i in range(steps_k):
        mask_ref[i] = (tile_start <= float(i)).astype(f32).astype(bf16)

    def chunk(c, norm):
        copy(c).wait()
        base = pl.multiple_of(c * rows, 8)
        acc = [jnp.zeros((8, paths), f32) for _ in range(rows // 8)]
        for i in range(steps_k):
            live = mask_ref[i]
            x = buf[i, pl.ds(base, rows), :]
            x = jnp.concatenate(
                [x[r : r + PACKED] * live[: min(PACKED, rows - r)] for r in range(0, rows, PACKED)],
                axis=0,
            )
            buf[i, pl.ds(base, rows), :] = x
            x = x.astype(f32)
            for r in range(rows // 8):
                acc[r] = acc[r] + x[8 * r : 8 * r + 8]
        root = jnp.sqrt(jnp.float32(step_len))
        for r in range(rows // 8):
            end = root * acc[r]
            end_ref[pl.ds(pl.multiple_of(base + 8 * r, 8), 8), :] = end
            norm = norm + end * end
        return norm

    norm = lax.fori_loop(0, chunks, chunk, jnp.zeros((8, paths), f32))
    full = end_ref.shape[0]
    end_ref[width:full, :] = jnp.zeros((full - width, paths), f32)
    value = 1.0 / (2.0 + 0.4 * jnp.sum(norm, axis=0, keepdims=True) / width)
    first = jnp.where(level == 0.0, value, 0.0)
    remaining = horizon - start_t * step_len
    coef = share / remaining
    hot = start_hot(start_t, steps_k)
    rows_ref[...] = jnp.concatenate(
        [level, start_t, first, share, coef, jnp.zeros((3, paths), f32)], axis=0
    )
    half = mine_ref.shape[1]

    def store(c, tile):
        side, at = divmod(c * LANES, half)
        part_ref[side, :, at : at + LANES] = tile

    weighted_sums(end_ref, store, hot, coef * first, share * first, width, split3)
    side = my_side()
    mine_ref[...] = part_ref[side]
    other_ref[...] = part_ref[1 - side]


def dots_over(z_half, buf, begin, end):
    steps_k, paths = buf.shape[0], buf.shape[2]
    later = lax.broadcasted_iota(i32, (steps_k, LANES), 0)
    total = jnp.zeros((steps_k, paths), f32)
    for i in range(steps_k - 1):
        open_rows = (later > i).astype(f32).astype(bf16)
        z_open = [
            z_half[:, c : c + LANES] * open_rows for c in range(0, z_half.shape[1], LANES)
        ]
        z_open = jnp.concatenate(z_open, axis=1)[:, : end - begin]
        total = total + dot(z_open, buf[i, begin:end, :])
    return total


def half_dots(z_half, side, buf, total_ref):
    width, half = buf.shape[1], z_half.shape[1]
    for which, begin, end in ((0, 0, min(half, width)), (1, half, width)):

        @pl.when(side == which)
        def _(begin=begin, end=end):
            total_ref[...] = dots_over(z_half, buf, begin, end)


def own_half_kernel(buf, z_ref, total_ref):
    half_dots(z_ref[...], my_side(), buf, total_ref)


def second_kernel(
    n_tm, buf, mine_ref, other_ref, total_ref, end_ref, rows_ref, *refs
):
    *out_refs, z_ref, part_ref, rest_ref = refs
    steps_k, width, paths = buf.shape
    step_len = horizon / steps_k
    half = mine_ref.shape[1]
    group = steps_k // n_tm
    side = my_side()
    half_dots(other_ref[...], 1 - side, buf, rest_ref)
    z_ref[side] = mine_ref[...].astype(f32)
    z_ref[1 - side] = other_ref[...].astype(f32)
    value_one = sum(
        z_ref[1, :, width + r - half : width + r - half + 1] for r in range(VALUE_COPIES)
    )
    level, start_t, first, share, coef = (rows_ref[r : r + 1, :] for r in range(5))
    at = lax.broadcasted_iota(i32, (steps_k, paths), 0)

    total = total_ref[...] + rest_ref[...]
    estimate = value_one + jnp.sqrt(jnp.float32(step_len)) * total
    drift = estimate - estimate * estimate * estimate
    lvl = level.astype(i32)
    fine = lax.shift_left(jnp.ones_like(lvl), LEVELS - 1 - lvl)
    on_fine = (at & (fine - 1)) == 0
    on_coarse = ((at & (2 * fine - 1)) == 0) & (lvl > 0)
    weight = jnp.where(on_fine, fine, 0) - jnp.where(on_coarse, 2 * fine, 0)
    weight = jnp.where(at.astype(f32) >= start_t, weight.astype(f32), 0.0) * step_len
    second = first + jnp.sum(weight * drift, axis=0, keepdims=True)
    hot = start_hot(start_t, steps_k)

    def store(c, tile):
        part_ref[:, c * LANES : (c + 1) * LANES] = tile

    weighted_sums(end_ref, store, hot, coef * second, share * second, width, split2)
    me = lax.axis_index("tm")
    for away, out_ref in enumerate(out_refs):
        out_ref[...] = part_ref[pl.ds(pl.multiple_of((me ^ away) * group, group), group), :]


def last_kernel(width, *refs):
    *parts, value_ref, grad_ref, value_buf, grad_buf, sems = refs
    total = pairwise([part[...] for part in parts])
    group = total.shape[0]
    grad_buf[...] = total[:, :width]
    square = (group, group)
    eye = lax.broadcasted_iota(i32, square, 0) == lax.broadcasted_iota(i32, square, 1)
    column = jnp.broadcast_to(total[:, width : width + 1], square)
    value_buf[...] = jnp.sum(jnp.where(eye, column, 0.0), axis=0, keepdims=True)
    copies = [
        pltpu.make_async_copy(grad_buf, grad_ref, sems.at[0]),
        pltpu.make_async_copy(value_buf, value_ref, sems.at[1]),
    ]
    for copy in copies:
        copy.start()
    for copy in copies:
        copy.wait()


def params():
    return pltpu.CompilerParams(vmem_limit_bytes=VMEM_LIMIT)


def in_hbm(x):
    return pltpu.with_memory_space_constraint(x, pltpu.HBM)


def swap(x, flips, odd_flips=None):
    n_tm = lax.axis_size("tm")
    even, odd = (path * n_tm + tm for path, tm in (flips, odd_flips or flips))
    pairs = [
        (i, i ^ (odd if i // n_tm % 2 else even)) for i in range(lax.axis_size(("path", "tm")))
    ]
    return lax.ppermute(x, ("path", "tm"), pairs)


def my_side():
    return lax.axis_index("path") & 1


def add_kernel(*refs):
    *parts, out_ref = refs
    out_ref[...] = pairwise([part[...] for part in parts])


def round_kernel(width, *refs):
    *parts, out_ref = refs
    total = pairwise([part[...] for part in parts])
    first = my_side() * total.shape[1] - width
    column = lax.broadcasted_iota(i32, total.shape, 1) + first
    high, middle, low = (part.astype(f32) for part in split3(total))
    out_ref[...] = jnp.where(column == 1, middle, jnp.where(column == 2, low, high)).astype(bf16)


def pairwise(parts):
    while len(parts) > 1:
        parts = [a + b for a, b in zip(parts[::2], parts[1::2])]
    return parts[0]


def local(kernel, dtype, parts):
    vmem = pl.BlockSpec(memory_space=pltpu.VMEM)
    return pl.pallas_call(
        kernel,
        out_shape=jax.ShapeDtypeStruct(parts[0].shape, dtype),
        in_specs=[vmem] * len(parts),
        out_specs=vmem,
        compiler_params=pltpu.CompilerParams(vmem_limit_bytes=SMALL_LIMIT),
    )(*parts)


def path_steps(n_path):
    steps, bit = [], 2
    while bit < n_path:
        steps.append((bit, 2 * bit, 3 * bit) if 2 * bit < n_path else (bit,))
        bit *= 4
    return steps


def tm_steps(n_tm):
    return [tuple(step // 2 for step in steps) for steps in path_steps(2 * n_tm)]


def shards(n_path, n_tm, increments, level_table, time_table):
    paths, steps_k, width = increments.shape
    group = steps_k // n_tm
    full = round_up(width + VALUE_COPIES, 2 * LANES)
    half = full // 2
    inc = jnp.transpose(increments, (1, 2, 0))
    vmem = pl.BlockSpec(memory_space=pltpu.VMEM)
    hbm = pl.BlockSpec(memory_space=pltpu.HBM)
    chunks = width // chunk_rows(width)

    mine, other, end, rows, held = pl.pallas_call(
        functools.partial(first_kernel, n_path, n_tm),
        out_shape=(
            jax.ShapeDtypeStruct((steps_k, half), f32),
            jax.ShapeDtypeStruct((steps_k, half), f32),
            jax.ShapeDtypeStruct((full, paths), f32),
            jax.ShapeDtypeStruct((8, paths), f32),
            jax.ShapeDtypeStruct(inc.shape, bf16),
        ),
        in_specs=[hbm, hbm, hbm],
        out_specs=(vmem,) * 5,
        scratch_shapes=[
            pltpu.VMEM((1, level_table.shape[0]), i32),
            pltpu.VMEM((1, time_table.shape[0]), i32),
            pltpu.VMEM((2, steps_k, half), f32),
            pltpu.VMEM((steps_k, PACKED, paths), bf16),
            pltpu.SemaphoreType.DMA((chunks,)),
            pltpu.SemaphoreType.DMA((2,)),
        ],
        compiler_params=params(),
        name="first_iterate",
    )(inc, *(in_hbm(table.reshape(1, -1)) for table in (level_table, time_table)))

    parts = [mine, swap(other, (1, 0))]
    over_path = [[(flip, 0) for flip in step] for step in path_steps(n_path)]
    over_tm = [[(0, flip) for flip in step] for step in tm_steps(n_tm)]
    odd, even = over_tm + over_path, over_path + over_tm
    if [len(step) for step in even] != [len(step) for step in odd]:
        odd = even
    for even_step, odd_step in zip(even, odd):
        total = local(add_kernel, f32, parts)
        parts = [total] + [swap(total, *flips) for flips in zip(even_step, odd_step)]
    own = local(functools.partial(round_kernel, width), bf16, parts)

    other = swap(own, (1, 0))
    total = pl.pallas_call(
        own_half_kernel,
        out_shape=jax.ShapeDtypeStruct((steps_k, paths), f32),
        in_specs=[vmem] * 2,
        out_specs=vmem,
        compiler_params=params(),
        cost_estimate=pl.CostEstimate(
            flops=paths * steps_k * steps_k * width, bytes_accessed=0, transcendentals=0
        ),
        name="own_half",
    )(held, own)
    parts = pl.pallas_call(
        functools.partial(second_kernel, n_tm),
        out_shape=(jax.ShapeDtypeStruct((group, full), f32),) * n_tm,
        in_specs=[vmem] * 6,
        out_specs=(vmem,) * n_tm,
        scratch_shapes=[
            pltpu.VMEM((2, steps_k, half), f32),
            pltpu.VMEM((steps_k, full), f32),
            pltpu.VMEM((steps_k, paths), f32),
        ],
        compiler_params=params(),
        name="second_iterate",
    )(held, own, other, total, end, rows)

    own = pairwise([parts[0]] + [swap(parts[away], (1, away)) for away in range(1, n_tm)])
    parts = [own, swap(own, (1, 0))]
    for step in path_steps(n_path):
        total = pairwise(parts)
        parts = [total] + [swap(total, (flip + 1, 0)) for flip in step]
    value, grad = pl.pallas_call(
        functools.partial(last_kernel, width),
        out_shape=(
            jax.ShapeDtypeStruct((1, group), f32),
            jax.ShapeDtypeStruct((group, width), f32),
        ),
        in_specs=[vmem] * len(parts),
        out_specs=(hbm, hbm),
        scratch_shapes=[
            pltpu.VMEM((1, group), f32),
            pltpu.VMEM((group, width), f32),
            pltpu.SemaphoreType.DMA((2,)),
        ],
        compiler_params=pltpu.CompilerParams(vmem_limit_bytes=SMALL_LIMIT),
        name="last_sum",
    )(*parts)
    return value.reshape(group), grad


def solution(mesh):
    placed = (P(("path", "tm"), None, None), P(), P())
    return jax.shard_map(
        functools.partial(shards, mesh.shape["path"], mesh.shape["tm"]),
        mesh=mesh,
        in_specs=placed,
        out_specs=(P("tm"), P("tm", None)),
        check_vma=False,
    )
```

```python
import functools

import jax
import jax.numpy as jnp
from jax import lax
from jax.experimental import pallas as pl
from jax.experimental.pallas import tpu as pltpu
from jax.sharding import PartitionSpec as P

LEVELS = 5
BLOCK = 2
LANES = 128
VALUE_COPIES = 3
PACKED = 16
VMEM_LIMIT = 24 * 1024 * 1024
SMALL_LIMIT = 4 * 1024 * 1024

horizon = 0.3
f32, bf16, i32 = jnp.float32, jnp.bfloat16, jnp.int32


def round_up(value, unit):
    return -(-value // unit) * unit


def chunk_rows(width):
    return next(r for r in (40, 32, 48, 24, 16, 8) if width % r == 0)


def split3(x):
    hi = x.astype(bf16)
    rest = x - hi.astype(f32)
    mid = rest.astype(bf16)
    low = (rest - mid.astype(f32)).astype(bf16)
    return hi, mid, low


def split2(x):
    hi = x.astype(bf16)
    return hi, (x - hi.astype(f32)).astype(bf16)


def contract_last(a, b):
    return lax.dot_general(a, b, (((1,), (1,)), ((), ())), preferred_element_type=f32)


def dot(a, b):
    return jnp.dot(a, b, preferred_element_type=f32)


def path_rows(lvl_ref, time_ref, steps_k, blk_dev, my_block):
    paths = BLOCK * blk_dev
    blocks = lvl_ref.shape[1]
    start = pl.multiple_of(my_block, LANES)
    own = jnp.concatenate(
        [lvl_ref[:, pl.ds(start, blk_dev)], time_ref[:, pl.ds(start, blk_dev)]], axis=0
    ).astype(f32)
    own = jnp.concatenate([own, jnp.zeros((6, blk_dev), f32)], axis=0).astype(bf16)
    block_of = lax.broadcasted_iota(i32, (blk_dev, paths), 1) // BLOCK
    repeat = (block_of == lax.broadcasted_iota(i32, (blk_dev, paths), 0)).astype(f32).astype(bf16)
    both = dot(own, repeat)
    level, start_t = both[0:1], both[1:2]
    lvl_hot = (lax.broadcasted_iota(i32, (8, blocks), 0) == lvl_ref[...]).astype(f32).astype(bf16)
    time_hot = (
        (lax.broadcasted_iota(i32, (steps_k, blocks), 0) == time_ref[...]).astype(f32).astype(bf16)
    )
    counts = contract_last(lvl_hot, time_hot)
    high = jnp.floor(counts * (1.0 / 256.0))
    low = counts - 256.0 * high
    own_time = start_hot(start_t, steps_k)
    at_time = 256.0 * dot(high.astype(bf16), own_time) + dot(low.astype(bf16), own_time)
    own_lvl = lax.broadcasted_iota(i32, (8, paths), 0).astype(f32) == level
    count = jnp.sum(jnp.where(own_lvl, at_time, 0.0), axis=0, keepdims=True)
    return level, start_t, 1.0 / (BLOCK * count)


def start_hot(start_t, steps_k):
    rows = lax.broadcasted_iota(i32, (steps_k, start_t.shape[1]), 0).astype(f32)
    return (rows == start_t).astype(f32).astype(bf16)


def weighted_sums(end_ref, begin, out_ref, hot, coef, value_row, width, split):
    for c in range(0, out_ref.shape[1], LANES):
        y = end_ref[pl.ds(pl.multiple_of(begin + c, LANES), LANES), :] * coef
        row = lax.broadcasted_iota(i32, y.shape, 0) + (begin + c - width)
        if not isinstance(begin, int) or c + LANES > width - begin:
            y = jnp.where((row >= 0) & (row < VALUE_COPIES), value_row, y)
        out_ref[:, c : c + LANES] = sum(contract_last(hot, part) for part in split(y))


def first_kernel(
    n_path, n_tm, inc_ref, lvl_hbm, time_hbm, other_ref, end_ref, rows_ref, buf,
    lvl_ref, time_ref, mask_ref, sems, table_sems,
):
    steps_k, width, paths = inc_ref.shape
    blk_dev = paths // BLOCK
    step_len = horizon / steps_k
    rows = chunk_rows(width)
    chunks = width // rows

    def copy(c):
        part = pl.ds(pl.multiple_of(c * rows, 8), rows)
        return pltpu.make_async_copy(inc_ref.at[:, part, :], buf.at[:, part, :], sems.at[c])

    tables = [
        pltpu.make_async_copy(lvl_hbm, lvl_ref, table_sems.at[0]),
        pltpu.make_async_copy(time_hbm, time_ref, table_sems.at[1]),
    ]
    for table in tables:
        table.start()

    @pl.loop(0, chunks)
    def _(c):
        copy(c).start()

    for table in tables:
        table.wait()
    me = lax.axis_index("path") * n_tm + lax.axis_index("tm")
    level, start_t, share = path_rows(lvl_ref, time_ref, steps_k, blk_dev, me * blk_dev)
    tile_start = jnp.broadcast_to(start_t, (PACKED, paths))
    for i in range(steps_k):
        mask_ref[i] = (tile_start <= float(i)).astype(f32).astype(bf16)

    def chunk(c, norm):
        copy(c).wait()
        base = pl.multiple_of(c * rows, 8)
        acc = [jnp.zeros((8, paths), f32) for _ in range(rows // 8)]
        for i in range(steps_k):
            live = mask_ref[i]
            x = buf[i, pl.ds(base, rows), :]
            x = jnp.concatenate(
                [x[r : r + PACKED] * live[: min(PACKED, rows - r)] for r in range(0, rows, PACKED)],
                axis=0,
            )
            buf[i, pl.ds(base, rows), :] = x
            x = x.astype(f32)
            for r in range(rows // 8):
                acc[r] = acc[r] + x[8 * r : 8 * r + 8]
        root = jnp.sqrt(jnp.float32(step_len))
        for r in range(rows // 8):
            end = root * acc[r]
            end_ref[pl.ds(pl.multiple_of(base + 8 * r, 8), 8), :] = end
            norm = norm + end * end
        return norm

    norm = lax.fori_loop(0, chunks, chunk, jnp.zeros((8, paths), f32))
    full = end_ref.shape[0]
    end_ref[width:full, :] = jnp.zeros((full - width, paths), f32)
    value = 1.0 / (2.0 + 0.4 * jnp.sum(norm, axis=0, keepdims=True) / width)
    first = jnp.where(level == 0.0, value, 0.0)
    remaining = horizon - start_t * step_len
    coef = share / remaining
    hot = start_hot(start_t, steps_k)
    rows_ref[...] = jnp.concatenate(
        [level, start_t, first, share, coef, jnp.zeros((3, paths), f32)], axis=0
    )
    half = other_ref.shape[1]
    begin = (1 - my_side()) * half
    weighted_sums(end_ref, begin, other_ref, hot, coef * first, share * first, width, split3)


def own_sums_kernel(width, steps_k, end_ref, rows_ref, mine_ref):
    _, start_t, first, share, coef = (rows_ref[r : r + 1, :] for r in range(5))
    hot = start_hot(start_t, steps_k)
    begin = my_side() * mine_ref.shape[1]
    weighted_sums(end_ref, begin, mine_ref, hot, coef * first, share * first, width, split3)


def dots_over(z_half, buf, begin, end):
    steps_k, paths = buf.shape[0], buf.shape[2]
    later = lax.broadcasted_iota(i32, (steps_k, LANES), 0)
    total = jnp.zeros((steps_k, paths), f32)
    for i in range(steps_k - 1):
        open_rows = (later > i).astype(f32).astype(bf16)
        z_open = [
            z_half[:, c : c + LANES] * open_rows for c in range(0, z_half.shape[1], LANES)
        ]
        z_open = jnp.concatenate(z_open, axis=1)[:, : end - begin]
        total = total + dot(z_open, buf[i, begin:end, :])
    return total


def half_dots(z_half, side, buf, total_ref):
    width, half = buf.shape[1], z_half.shape[1]
    for which, begin, end in ((0, 0, min(half, width)), (1, half, width)):

        @pl.when(side == which)
        def _(begin=begin, end=end):
            total_ref[...] = dots_over(z_half, buf, begin, end)


def own_half_kernel(buf, z_ref, total_ref):
    half_dots(z_ref[...], my_side(), buf, total_ref)


def second_kernel(
    n_tm, buf, mine_ref, other_ref, total_ref, end_ref, rows_ref, *refs
):
    *out_refs, z_ref, part_ref, rest_ref = refs
    steps_k, width, paths = buf.shape
    step_len = horizon / steps_k
    half = mine_ref.shape[1]
    group = steps_k // n_tm
    side = my_side()
    half_dots(other_ref[...], 1 - side, buf, rest_ref)
    z_ref[side] = mine_ref[...].astype(f32)
    z_ref[1 - side] = other_ref[...].astype(f32)
    value_one = sum(
        z_ref[1, :, width + r - half : width + r - half + 1] for r in range(VALUE_COPIES)
    )
    level, start_t, first, share, coef = (rows_ref[r : r + 1, :] for r in range(5))
    at = lax.broadcasted_iota(i32, (steps_k, paths), 0)

    total = total_ref[...] + rest_ref[...]
    estimate = value_one + jnp.sqrt(jnp.float32(step_len)) * total
    drift = estimate - estimate * estimate * estimate
    lvl = level.astype(i32)
    fine = lax.shift_left(jnp.ones_like(lvl), LEVELS - 1 - lvl)
    on_fine = (at & (fine - 1)) == 0
    on_coarse = ((at & (2 * fine - 1)) == 0) & (lvl > 0)
    weight = jnp.where(on_fine, fine, 0) - jnp.where(on_coarse, 2 * fine, 0)
    weight = jnp.where(at.astype(f32) >= start_t, weight.astype(f32), 0.0) * step_len
    second = first + jnp.sum(weight * drift, axis=0, keepdims=True)
    hot = start_hot(start_t, steps_k)

    weighted_sums(end_ref, 0, part_ref, hot, coef * second, share * second, width, split2)
    me = lax.axis_index("tm")
    for away, out_ref in enumerate(out_refs):
        out_ref[...] = part_ref[pl.ds(pl.multiple_of((me ^ away) * group, group), group), :]


def last_kernel(width, *refs):
    *parts, value_ref, grad_ref, value_buf, grad_buf, sems = refs
    total = pairwise([part[...] for part in parts])
    group = total.shape[0]
    grad_buf[...] = total[:, :width]
    square = (group, group)
    eye = lax.broadcasted_iota(i32, square, 0) == lax.broadcasted_iota(i32, square, 1)
    column = jnp.broadcast_to(total[:, width : width + 1], square)
    value_buf[...] = jnp.sum(jnp.where(eye, column, 0.0), axis=0, keepdims=True)
    copies = [
        pltpu.make_async_copy(grad_buf, grad_ref, sems.at[0]),
        pltpu.make_async_copy(value_buf, value_ref, sems.at[1]),
    ]
    for copy in copies:
        copy.start()
    for copy in copies:
        copy.wait()


def params():
    return pltpu.CompilerParams(vmem_limit_bytes=VMEM_LIMIT)


def in_hbm(x):
    return pltpu.with_memory_space_constraint(x, pltpu.HBM)


def swap(x, flips, odd_flips=None):
    n_path, n_tm = lax.axis_size("path"), lax.axis_size("tm")
    even, odd = (path * n_tm + tm for path, tm in (flips, odd_flips or flips))
    pairs = [
        (i, i ^ (odd if side_of(i // n_tm, i % n_tm, n_path) else even))
        for i in range(lax.axis_size(("path", "tm")))
    ]
    return lax.ppermute(x, ("path", "tm"), pairs)


def parity(n):
    return bin(n).count("1") % 2


def side_of(path, tm, n_path):
    bits = tm
    for bit in range(n_path.bit_length() - 1):
        bits = bits + (path >> bit)
    return bits & 1


def my_side():
    return side_of(lax.axis_index("path"), lax.axis_index("tm"), lax.axis_size("path"))


def add_kernel(*refs):
    *parts, out_ref = refs
    out_ref[...] = pairwise([part[...] for part in parts])


def round_kernel(width, *refs):
    *parts, out_ref = refs
    total = pairwise([part[...] for part in parts])
    first = my_side() * total.shape[1] - width
    column = lax.broadcasted_iota(i32, total.shape, 1) + first
    high, middle, low = (part.astype(f32) for part in split3(total))
    out_ref[...] = jnp.where(column == 1, middle, jnp.where(column == 2, low, high)).astype(bf16)


def pairwise(parts):
    while len(parts) > 1:
        parts = [a + b for a, b in zip(parts[::2], parts[1::2])]
    return parts[0]


def local(kernel, dtype, parts):
    vmem = pl.BlockSpec(memory_space=pltpu.VMEM)
    return pl.pallas_call(
        kernel,
        out_shape=jax.ShapeDtypeStruct(parts[0].shape, dtype),
        in_specs=[vmem] * len(parts),
        out_specs=vmem,
        compiler_params=pltpu.CompilerParams(vmem_limit_bytes=SMALL_LIMIT),
    )(*parts)


def path_steps(n_path):
    steps, bit = [], 2
    while bit < n_path:
        steps.append((bit, 2 * bit, 3 * bit) if 2 * bit < n_path else (bit,))
        bit *= 4
    return steps


def tm_steps(n_tm):
    return [tuple(step // 2 for step in steps) for steps in path_steps(2 * n_tm)]


def shards(n_path, n_tm, increments, level_table, time_table):
    paths, steps_k, width = increments.shape
    group = steps_k // n_tm
    full = round_up(width + VALUE_COPIES, 2 * LANES)
    half = full // 2
    inc = jnp.transpose(increments, (1, 2, 0))
    vmem = pl.BlockSpec(memory_space=pltpu.VMEM)
    hbm = pl.BlockSpec(memory_space=pltpu.HBM)
    chunks = width // chunk_rows(width)

    other, end, rows, held = pl.pallas_call(
        functools.partial(first_kernel, n_path, n_tm),
        out_shape=(
            jax.ShapeDtypeStruct((steps_k, half), f32),
            jax.ShapeDtypeStruct((full, paths), f32),
            jax.ShapeDtypeStruct((8, paths), f32),
            jax.ShapeDtypeStruct(inc.shape, bf16),
        ),
        in_specs=[hbm, hbm, hbm],
        out_specs=(vmem,) * 4,
        scratch_shapes=[
            pltpu.VMEM((1, level_table.shape[0]), i32),
            pltpu.VMEM((1, time_table.shape[0]), i32),
            pltpu.VMEM((steps_k, PACKED, paths), bf16),
            pltpu.SemaphoreType.DMA((chunks,)),
            pltpu.SemaphoreType.DMA((2,)),
        ],
        compiler_params=params(),
        name="first_iterate",
    )(inc, *(in_hbm(table.reshape(1, -1)) for table in (level_table, time_table)))

    other = swap(other, (1, 0))
    mine = pl.pallas_call(
        functools.partial(own_sums_kernel, width, steps_k),
        out_shape=jax.ShapeDtypeStruct((steps_k, half), f32),
        in_specs=[vmem] * 2,
        out_specs=vmem,
        compiler_params=pltpu.CompilerParams(vmem_limit_bytes=SMALL_LIMIT),
        cost_estimate=pl.CostEstimate(
            flops=6 * steps_k * half * paths, bytes_accessed=0, transcendentals=0
        ),
        name="own_sums",
    )(end, rows)
    parts = [mine, other]
    over_path = [[(flip + parity(flip), 0) for flip in step] for step in path_steps(n_path)]
    over_tm = [[(flip % 2, flip) for flip in step] for step in tm_steps(n_tm)]
    odd, even = over_tm + over_path, over_path + over_tm
    if [len(step) for step in even] != [len(step) for step in odd]:
        odd = even
    for even_step, odd_step in zip(even, odd):
        total = local(add_kernel, f32, parts)
        parts = [total] + [swap(total, *flips) for flips in zip(even_step, odd_step)]
    own = local(functools.partial(round_kernel, width), bf16, parts)

    other = swap(own, (1, 0))
    total = pl.pallas_call(
        own_half_kernel,
        out_shape=jax.ShapeDtypeStruct((steps_k, paths), f32),
        in_specs=[vmem] * 2,
        out_specs=vmem,
        compiler_params=params(),
        cost_estimate=pl.CostEstimate(
            flops=paths * steps_k * steps_k * width, bytes_accessed=0, transcendentals=0
        ),
        name="own_half",
    )(held, own)
    parts = pl.pallas_call(
        functools.partial(second_kernel, n_tm),
        out_shape=(jax.ShapeDtypeStruct((group, full), f32),) * n_tm,
        in_specs=[vmem] * 6,
        out_specs=(vmem,) * n_tm,
        scratch_shapes=[
            pltpu.VMEM((2, steps_k, half), f32),
            pltpu.VMEM((steps_k, full), f32),
            pltpu.VMEM((steps_k, paths), f32),
        ],
        compiler_params=params(),
        name="second_iterate",
    )(held, own, other, total, end, rows)

    own = pairwise([parts[0]] + [swap(parts[away], (1, away)) for away in range(1, n_tm)])
    parts = [own, swap(own, (1, 0))]
    for step in path_steps(n_path):
        total = pairwise(parts)
        parts = [total] + [swap(total, (flip + 1, 0)) for flip in step]
    value, grad = pl.pallas_call(
        functools.partial(last_kernel, width),
        out_shape=(
            jax.ShapeDtypeStruct((1, group), f32),
            jax.ShapeDtypeStruct((group, width), f32),
        ),
        in_specs=[vmem] * len(parts),
        out_specs=(hbm, hbm),
        scratch_shapes=[
            pltpu.VMEM((1, group), f32),
            pltpu.VMEM((group, width), f32),
            pltpu.SemaphoreType.DMA((2,)),
        ],
        compiler_params=pltpu.CompilerParams(vmem_limit_bytes=SMALL_LIMIT),
        name="last_sum",
    )(*parts)
    return value.reshape(group), grad


def solution(mesh):
    placed = (P(("path", "tm"), None, None), P(), P())
    return jax.shard_map(
        functools.partial(shards, mesh.shape["path"], mesh.shape["tm"]),
        mesh=mesh,
        in_specs=placed,
        out_specs=(P("tm"), P("tm", None)),
        check_vma=False,
    )
```

```python
import functools

import jax
import jax.numpy as jnp
from jax import lax
from jax.experimental import pallas as pl
from jax.experimental.pallas import tpu as pltpu
from jax.sharding import PartitionSpec as P

LEVELS = 5
BLOCK = 2
LANES = 128
VALUE_COPIES = 3
PACKED = 16
VMEM_LIMIT = 24 * 1024 * 1024
SMALL_LIMIT = 4 * 1024 * 1024

horizon = 0.3
f32, bf16, i32 = jnp.float32, jnp.bfloat16, jnp.int32


def round_up(value, unit):
    return -(-value // unit) * unit


def chunk_rows(width):
    return next(r for r in (40, 32, 48, 24, 16, 8) if width % r == 0)


def split3(x):
    hi = x.astype(bf16)
    rest = x - hi.astype(f32)
    mid = rest.astype(bf16)
    low = (rest - mid.astype(f32)).astype(bf16)
    return hi, mid, low


def split2(x):
    hi = x.astype(bf16)
    return hi, (x - hi.astype(f32)).astype(bf16)


def contract_last(a, b):
    return lax.dot_general(a, b, (((1,), (1,)), ((), ())), preferred_element_type=f32)


def dot(a, b):
    return jnp.dot(a, b, preferred_element_type=f32)


def path_rows(lvl_ref, time_ref, steps_k, blk_dev, my_block):
    paths = BLOCK * blk_dev
    blocks = lvl_ref.shape[1]
    start = pl.multiple_of(my_block, LANES)
    own = jnp.concatenate(
        [lvl_ref[:, pl.ds(start, blk_dev)], time_ref[:, pl.ds(start, blk_dev)]], axis=0
    ).astype(f32)
    own = jnp.concatenate([own, jnp.zeros((6, blk_dev), f32)], axis=0).astype(bf16)
    block_of = lax.broadcasted_iota(i32, (blk_dev, paths), 1) // BLOCK
    repeat = (block_of == lax.broadcasted_iota(i32, (blk_dev, paths), 0)).astype(f32).astype(bf16)
    both = dot(own, repeat)
    level, start_t = both[0:1], both[1:2]
    lvl_hot = (lax.broadcasted_iota(i32, (8, blocks), 0) == lvl_ref[...]).astype(f32).astype(bf16)
    time_hot = (
        (lax.broadcasted_iota(i32, (steps_k, blocks), 0) == time_ref[...]).astype(f32).astype(bf16)
    )
    counts = contract_last(lvl_hot, time_hot)
    high = jnp.floor(counts * (1.0 / 256.0))
    low = counts - 256.0 * high
    own_time = start_hot(start_t, steps_k)
    at_time = 256.0 * dot(high.astype(bf16), own_time) + dot(low.astype(bf16), own_time)
    own_lvl = lax.broadcasted_iota(i32, (8, paths), 0).astype(f32) == level
    count = jnp.sum(jnp.where(own_lvl, at_time, 0.0), axis=0, keepdims=True)
    return level, start_t, 1.0 / (BLOCK * count)


def start_hot(start_t, steps_k):
    rows = lax.broadcasted_iota(i32, (steps_k, start_t.shape[1]), 0).astype(f32)
    return (rows == start_t).astype(f32).astype(bf16)


def weighted_sums(end_ref, begin, out_ref, hot, coef, value_row, width, split):
    for c in range(0, out_ref.shape[1], LANES):
        y = end_ref[pl.ds(pl.multiple_of(begin + c, LANES), LANES), :] * coef
        row = lax.broadcasted_iota(i32, y.shape, 0) + (begin + c - width)
        if not isinstance(begin, int) or c + LANES > width - begin:
            y = jnp.where((row >= 0) & (row < VALUE_COPIES), value_row, y)
        out_ref[:, c : c + LANES] = sum(contract_last(hot, part) for part in split(y))


def first_kernel(
    n_path, n_tm, inc_ref, lvl_hbm, time_hbm, other_ref, end_ref, rows_ref, buf,
    lvl_ref, time_ref, mask_ref, sems, table_sems,
):
    steps_k, width, paths = inc_ref.shape
    blk_dev = paths // BLOCK
    step_len = horizon / steps_k
    rows = chunk_rows(width)
    chunks = width // rows

    def copy(c):
        part = pl.ds(pl.multiple_of(c * rows, 8), rows)
        return pltpu.make_async_copy(inc_ref.at[:, part, :], buf.at[:, part, :], sems.at[c])

    tables = [
        pltpu.make_async_copy(lvl_hbm, lvl_ref, table_sems.at[0]),
        pltpu.make_async_copy(time_hbm, time_ref, table_sems.at[1]),
    ]
    for table in tables:
        table.start()

    @pl.loop(0, chunks)
    def _(c):
        copy(c).start()

    for table in tables:
        table.wait()
    me = lax.axis_index("path") * n_tm + lax.axis_index("tm")
    level, start_t, share = path_rows(lvl_ref, time_ref, steps_k, blk_dev, me * blk_dev)
    tile_start = jnp.broadcast_to(start_t, (PACKED, paths))
    for i in range(steps_k):
        mask_ref[i] = (tile_start <= float(i)).astype(f32).astype(bf16)

    def chunk(c, norm):
        copy(c).wait()
        base = pl.multiple_of(c * rows, 8)
        acc = [jnp.zeros((8, paths), f32) for _ in range(rows // 8)]
        for i in range(steps_k):
            live = mask_ref[i]
            x = buf[i, pl.ds(base, rows), :]
            x = jnp.concatenate(
                [x[r : r + PACKED] * live[: min(PACKED, rows - r)] for r in range(0, rows, PACKED)],
                axis=0,
            )
            buf[i, pl.ds(base, rows), :] = x
            x = x.astype(f32)
            for r in range(rows // 8):
                acc[r] = acc[r] + x[8 * r : 8 * r + 8]
        root = jnp.sqrt(jnp.float32(step_len))
        for r in range(rows // 8):
            end = root * acc[r]
            end_ref[pl.ds(pl.multiple_of(base + 8 * r, 8), 8), :] = end
            norm = norm + end * end
        return norm

    norm = lax.fori_loop(0, chunks, chunk, jnp.zeros((8, paths), f32))
    full = end_ref.shape[0]
    end_ref[width:full, :] = jnp.zeros((full - width, paths), f32)
    value = 1.0 / (2.0 + 0.4 * jnp.sum(norm, axis=0, keepdims=True) / width)
    first = jnp.where(level == 0.0, value, 0.0)
    remaining = horizon - start_t * step_len
    coef = share / remaining
    hot = start_hot(start_t, steps_k)
    rows_ref[...] = jnp.concatenate(
        [level, start_t, first, share, coef, jnp.zeros((3, paths), f32)], axis=0
    )
    half = other_ref.shape[1]
    begin = (1 - my_side()) * half
    weighted_sums(end_ref, begin, other_ref, hot, coef * first, share * first, width, split3)


def own_sums_kernel(width, steps_k, end_ref, rows_ref, mine_ref):
    _, start_t, first, share, coef = (rows_ref[r : r + 1, :] for r in range(5))
    hot = start_hot(start_t, steps_k)
    begin = my_side() * mine_ref.shape[1]
    weighted_sums(end_ref, begin, mine_ref, hot, coef * first, share * first, width, split3)


def dots_over(z_half, buf, begin, end):
    steps_k, paths = buf.shape[0], buf.shape[2]
    later = lax.broadcasted_iota(i32, (steps_k, LANES), 0)
    total = jnp.zeros((steps_k, paths), f32)
    for i in range(steps_k - 1):
        open_rows = (later > i).astype(f32).astype(bf16)
        z_open = [
            z_half[:, c : c + LANES] * open_rows for c in range(0, z_half.shape[1], LANES)
        ]
        z_open = jnp.concatenate(z_open, axis=1)[:, : end - begin]
        total = total + dot(z_open, buf[i, begin:end, :])
    return total


def half_dots(z_half, side, buf, total_ref):
    width, half = buf.shape[1], z_half.shape[1]
    for which, begin, end in ((0, 0, min(half, width)), (1, half, width)):

        @pl.when(side == which)
        def _(begin=begin, end=end):
            total_ref[...] = dots_over(z_half, buf, begin, end)


def own_half_kernel(buf, z_ref, total_ref):
    half_dots(z_ref[...], my_side(), buf, total_ref)


def second_kernel(
    n_tm, buf, mine_ref, other_ref, total_ref, end_ref, rows_ref, *refs
):
    *out_refs, z_ref, part_ref, rest_ref = refs
    steps_k, width, paths = buf.shape
    step_len = horizon / steps_k
    half = mine_ref.shape[1]
    group = steps_k // n_tm
    side = my_side()
    half_dots(other_ref[...], 1 - side, buf, rest_ref)
    z_ref[side] = mine_ref[...].astype(f32)
    z_ref[1 - side] = other_ref[...].astype(f32)
    value_one = sum(
        z_ref[1, :, width + r - half : width + r - half + 1] for r in range(VALUE_COPIES)
    )
    level, start_t, first, share, coef = (rows_ref[r : r + 1, :] for r in range(5))
    at = lax.broadcasted_iota(i32, (steps_k, paths), 0)

    total = total_ref[...] + rest_ref[...]
    estimate = value_one + jnp.sqrt(jnp.float32(step_len)) * total
    drift = estimate - estimate * estimate * estimate
    lvl = level.astype(i32)
    fine = lax.shift_left(jnp.ones_like(lvl), LEVELS - 1 - lvl)
    on_fine = (at & (fine - 1)) == 0
    on_coarse = ((at & (2 * fine - 1)) == 0) & (lvl > 0)
    weight = jnp.where(on_fine, fine, 0) - jnp.where(on_coarse, 2 * fine, 0)
    weight = jnp.where(at.astype(f32) >= start_t, weight.astype(f32), 0.0) * step_len
    second = first + jnp.sum(weight * drift, axis=0, keepdims=True)
    hot = start_hot(start_t, steps_k)

    weighted_sums(end_ref, 0, part_ref, hot, coef * second, share * second, width, split2)
    me = lax.axis_index("tm")
    for away, out_ref in enumerate(out_refs):
        out_ref[...] = part_ref[pl.ds(pl.multiple_of((me ^ away) * group, group), group), :]


def last_kernel(width, *refs):
    *parts, value_ref, grad_ref, value_buf, grad_buf, sems = refs
    total = pairwise([part[...] for part in parts])
    group = total.shape[0]
    grad_buf[...] = total[:, :width]
    square = (group, group)
    eye = lax.broadcasted_iota(i32, square, 0) == lax.broadcasted_iota(i32, square, 1)
    column = jnp.broadcast_to(total[:, width : width + 1], square)
    value_buf[...] = jnp.sum(jnp.where(eye, column, 0.0), axis=0, keepdims=True)
    copies = [
        pltpu.make_async_copy(grad_buf, grad_ref, sems.at[0]),
        pltpu.make_async_copy(value_buf, value_ref, sems.at[1]),
    ]
    for copy in copies:
        copy.start()
    for copy in copies:
        copy.wait()


def params():
    return pltpu.CompilerParams(vmem_limit_bytes=VMEM_LIMIT)


def in_hbm(x):
    return pltpu.with_memory_space_constraint(x, pltpu.HBM)


def swap(x, flips, odd_flips=None):
    n_path, n_tm = lax.axis_size("path"), lax.axis_size("tm")
    even, odd = (path * n_tm + tm for path, tm in (flips, odd_flips or flips))
    pairs = [
        (i, i ^ (odd if side_of(i // n_tm, i % n_tm, n_path) else even))
        for i in range(lax.axis_size(("path", "tm")))
    ]
    return lax.ppermute(x, ("path", "tm"), pairs)


def parity(n):
    return bin(n).count("1") % 2


def side_of(path, tm, n_path):
    bits = tm
    for bit in range(n_path.bit_length() - 1):
        bits = bits + (path >> bit)
    return bits & 1


def my_side():
    return side_of(lax.axis_index("path"), lax.axis_index("tm"), lax.axis_size("path"))


def add_kernel(*refs):
    *parts, out_ref = refs
    out_ref[...] = pairwise([part[...] for part in parts])


def round_kernel(width, *refs):
    *parts, out_ref = refs
    total = pairwise([part[...] for part in parts])
    first = my_side() * total.shape[1] - width
    column = lax.broadcasted_iota(i32, total.shape, 1) + first
    high, middle, low = (part.astype(f32) for part in split3(total))
    out_ref[...] = jnp.where(column == 1, middle, jnp.where(column == 2, low, high)).astype(bf16)


def pairwise(parts):
    while len(parts) > 1:
        parts = [a + b for a, b in zip(parts[::2], parts[1::2])]
    return parts[0]


def local(kernel, dtype, parts):
    vmem = pl.BlockSpec(memory_space=pltpu.VMEM)
    return pl.pallas_call(
        kernel,
        out_shape=jax.ShapeDtypeStruct(parts[0].shape, dtype),
        in_specs=[vmem] * len(parts),
        out_specs=vmem,
        compiler_params=pltpu.CompilerParams(vmem_limit_bytes=SMALL_LIMIT),
    )(*parts)


def path_steps(n_path):
    steps, bit = [], 2
    while bit < n_path:
        steps.append((bit, 2 * bit, 3 * bit) if 2 * bit < n_path else (bit,))
        bit *= 4
    return steps


def tm_steps(n_tm):
    steps = [tuple(flip // 2 for flip in step) for step in path_steps(2 * n_tm)]
    return [(step[0], *step[:0:-1]) for step in steps]


def shards(n_path, n_tm, increments, level_table, time_table):
    paths, steps_k, width = increments.shape
    group = steps_k // n_tm
    full = round_up(width + VALUE_COPIES, 2 * LANES)
    half = full // 2
    inc = jnp.transpose(increments, (1, 2, 0))
    vmem = pl.BlockSpec(memory_space=pltpu.VMEM)
    hbm = pl.BlockSpec(memory_space=pltpu.HBM)
    chunks = width // chunk_rows(width)

    other, end, rows, held = pl.pallas_call(
        functools.partial(first_kernel, n_path, n_tm),
        out_shape=(
            jax.ShapeDtypeStruct((steps_k, half), f32),
            jax.ShapeDtypeStruct((full, paths), f32),
            jax.ShapeDtypeStruct((8, paths), f32),
            jax.ShapeDtypeStruct(inc.shape, bf16),
        ),
        in_specs=[hbm, hbm, hbm],
        out_specs=(vmem,) * 4,
        scratch_shapes=[
            pltpu.VMEM((1, level_table.shape[0]), i32),
            pltpu.VMEM((1, time_table.shape[0]), i32),
            pltpu.VMEM((steps_k, PACKED, paths), bf16),
            pltpu.SemaphoreType.DMA((chunks,)),
            pltpu.SemaphoreType.DMA((2,)),
        ],
        compiler_params=params(),
        name="first_iterate",
    )(inc, *(in_hbm(table.reshape(1, -1)) for table in (level_table, time_table)))

    other = swap(other, (1, 0))
    mine = pl.pallas_call(
        functools.partial(own_sums_kernel, width, steps_k),
        out_shape=jax.ShapeDtypeStruct((steps_k, half), f32),
        in_specs=[vmem] * 2,
        out_specs=vmem,
        compiler_params=pltpu.CompilerParams(vmem_limit_bytes=SMALL_LIMIT),
        cost_estimate=pl.CostEstimate(
            flops=6 * steps_k * half * paths, bytes_accessed=0, transcendentals=0
        ),
        name="own_sums",
    )(end, rows)
    parts = [mine, other]
    over_path = [[(flip + parity(flip), 0) for flip in step] for step in path_steps(n_path)]
    over_tm = [[(flip % 2, flip) for flip in step] for step in tm_steps(n_tm)]
    odd, even = over_tm + over_path, over_path + over_tm
    if [len(step) for step in even] != [len(step) for step in odd]:
        odd = even
    for even_step, odd_step in zip(even, odd):
        total = local(add_kernel, f32, parts)
        parts = [total] + [swap(total, *flips) for flips in zip(even_step, odd_step)]
    own = local(functools.partial(round_kernel, width), bf16, parts)

    other = swap(own, (1, 0))
    total = pl.pallas_call(
        own_half_kernel,
        out_shape=jax.ShapeDtypeStruct((steps_k, paths), f32),
        in_specs=[vmem] * 2,
        out_specs=vmem,
        compiler_params=params(),
        cost_estimate=pl.CostEstimate(
            flops=paths * steps_k * steps_k * width, bytes_accessed=0, transcendentals=0
        ),
        name="own_half",
    )(held, own)
    parts = pl.pallas_call(
        functools.partial(second_kernel, n_tm),
        out_shape=(jax.ShapeDtypeStruct((group, full), f32),) * n_tm,
        in_specs=[vmem] * 6,
        out_specs=(vmem,) * n_tm,
        scratch_shapes=[
            pltpu.VMEM((2, steps_k, half), f32),
            pltpu.VMEM((steps_k, full), f32),
            pltpu.VMEM((steps_k, paths), f32),
        ],
        compiler_params=params(),
        name="second_iterate",
    )(held, own, other, total, end, rows)

    order = [away for away in (*range(2, n_tm), 1) if away < n_tm]
    own = pairwise([parts[0]] + [swap(parts[away], (1, away)) for away in order])
    parts = [own, swap(own, (1, 0))]
    for step in path_steps(n_path):
        total = pairwise(parts)
        parts = [total] + [swap(total, (flip + 1, 0)) for flip in step]
    value, grad = pl.pallas_call(
        functools.partial(last_kernel, width),
        out_shape=(
            jax.ShapeDtypeStruct((1, group), f32),
            jax.ShapeDtypeStruct((group, width), f32),
        ),
        in_specs=[vmem] * len(parts),
        out_specs=(hbm, hbm),
        scratch_shapes=[
            pltpu.VMEM((1, group), f32),
            pltpu.VMEM((group, width), f32),
            pltpu.SemaphoreType.DMA((2,)),
        ],
        compiler_params=pltpu.CompilerParams(vmem_limit_bytes=SMALL_LIMIT),
        name="last_sum",
    )(*parts)
    return value.reshape(group), grad


def solution(mesh):
    placed = (P(("path", "tm"), None, None), P(), P())
    return jax.shard_map(
        functools.partial(shards, mesh.shape["path"], mesh.shape["tm"]),
        mesh=mesh,
        in_specs=placed,
        out_specs=(P("tm"), P("tm", None)),
        check_vma=False,
    )
```

```python
import functools

import jax
import jax.numpy as jnp
from jax import lax
from jax.experimental import pallas as pl
from jax.experimental.pallas import tpu as pltpu
from jax.sharding import PartitionSpec as P

LEVELS = 5
BLOCK = 2
LANES = 128
VALUE_COPIES = 3
PACKED = 16
VMEM_LIMIT = 24 * 1024 * 1024
SMALL_LIMIT = 4 * 1024 * 1024

horizon = 0.3
f32, bf16, i32 = jnp.float32, jnp.bfloat16, jnp.int32


def round_up(value, unit):
    return -(-value // unit) * unit


def chunk_rows(width):
    return next(r for r in (40, 32, 48, 24, 16, 8) if width % r == 0)


def split3(x):
    hi = x.astype(bf16)
    rest = x - hi.astype(f32)
    mid = rest.astype(bf16)
    low = (rest - mid.astype(f32)).astype(bf16)
    return hi, mid, low


def split2(x):
    hi = x.astype(bf16)
    return hi, (x - hi.astype(f32)).astype(bf16)


def contract_last(a, b):
    return lax.dot_general(a, b, (((1,), (1,)), ((), ())), preferred_element_type=f32)


def dot(a, b):
    return jnp.dot(a, b, preferred_element_type=f32)


def path_rows(lvl_ref, time_ref, steps_k, blk_dev, my_block):
    paths = BLOCK * blk_dev
    blocks = lvl_ref.shape[1]
    start = pl.multiple_of(my_block, LANES)
    own = jnp.concatenate(
        [lvl_ref[:, pl.ds(start, blk_dev)], time_ref[:, pl.ds(start, blk_dev)]], axis=0
    ).astype(f32)
    own = jnp.concatenate([own, jnp.zeros((6, blk_dev), f32)], axis=0).astype(bf16)
    block_of = lax.broadcasted_iota(i32, (blk_dev, paths), 1) // BLOCK
    repeat = (block_of == lax.broadcasted_iota(i32, (blk_dev, paths), 0)).astype(f32).astype(bf16)
    both = dot(own, repeat)
    level, start_t = both[0:1], both[1:2]
    lvl_hot = (lax.broadcasted_iota(i32, (8, blocks), 0) == lvl_ref[...]).astype(f32).astype(bf16)
    time_hot = (
        (lax.broadcasted_iota(i32, (steps_k, blocks), 0) == time_ref[...]).astype(f32).astype(bf16)
    )
    counts = contract_last(lvl_hot, time_hot)
    high = jnp.floor(counts * (1.0 / 256.0))
    low = counts - 256.0 * high
    own_time = start_hot(start_t, steps_k)
    at_time = 256.0 * dot(high.astype(bf16), own_time) + dot(low.astype(bf16), own_time)
    own_lvl = lax.broadcasted_iota(i32, (8, paths), 0).astype(f32) == level
    count = jnp.sum(jnp.where(own_lvl, at_time, 0.0), axis=0, keepdims=True)
    return level, start_t, 1.0 / (BLOCK * count)


def start_hot(start_t, steps_k):
    rows = lax.broadcasted_iota(i32, (steps_k, start_t.shape[1]), 0).astype(f32)
    return (rows == start_t).astype(f32).astype(bf16)


def weighted_sums(end_ref, begin, out_ref, hot, coef, value_row, width, split):
    for c in range(0, out_ref.shape[1], LANES):
        y = end_ref[pl.ds(pl.multiple_of(begin + c, LANES), LANES), :] * coef
        row = lax.broadcasted_iota(i32, y.shape, 0) + (begin + c - width)
        if not isinstance(begin, int) or c + LANES > width - begin:
            y = jnp.where((row >= 0) & (row < VALUE_COPIES), value_row, y)
        out_ref[:, c : c + LANES] = sum(contract_last(hot, part) for part in split(y))


def first_kernel(
    n_path, n_tm, inc_ref, lvl_hbm, time_hbm, other_ref, end_ref, rows_ref, buf,
    lvl_ref, time_ref, mask_ref, sems, table_sems,
):
    steps_k, width, paths = inc_ref.shape
    blk_dev = paths // BLOCK
    step_len = horizon / steps_k
    rows = chunk_rows(width)
    chunks = width // rows

    def copy(c):
        part = pl.ds(pl.multiple_of(c * rows, 8), rows)
        return pltpu.make_async_copy(inc_ref.at[:, part, :], buf.at[:, part, :], sems.at[c])

    tables = [
        pltpu.make_async_copy(lvl_hbm, lvl_ref, table_sems.at[0]),
        pltpu.make_async_copy(time_hbm, time_ref, table_sems.at[1]),
    ]
    for table in tables:
        table.start()

    @pl.loop(0, chunks)
    def _(c):
        copy(c).start()

    for table in tables:
        table.wait()
    me = lax.axis_index("path") * n_tm + lax.axis_index("tm")
    level, start_t, share = path_rows(lvl_ref, time_ref, steps_k, blk_dev, me * blk_dev)
    tile_start = jnp.broadcast_to(start_t, (PACKED, paths))
    for i in range(steps_k):
        mask_ref[i] = (tile_start <= float(i)).astype(f32).astype(bf16)

    def chunk(c, norm):
        copy(c).wait()
        base = pl.multiple_of(c * rows, 8)
        acc = [jnp.zeros((8, paths), f32) for _ in range(rows // 8)]
        for i in range(steps_k):
            live = mask_ref[i]
            x = buf[i, pl.ds(base, rows), :]
            x = jnp.concatenate(
                [x[r : r + PACKED] * live[: min(PACKED, rows - r)] for r in range(0, rows, PACKED)],
                axis=0,
            )
            buf[i, pl.ds(base, rows), :] = x
            x = x.astype(f32)
            for r in range(rows // 8):
                acc[r] = acc[r] + x[8 * r : 8 * r + 8]
        root = jnp.sqrt(jnp.float32(step_len))
        for r in range(rows // 8):
            end = root * acc[r]
            end_ref[pl.ds(pl.multiple_of(base + 8 * r, 8), 8), :] = end
            norm = norm + end * end
        return norm

    norm = lax.fori_loop(0, chunks, chunk, jnp.zeros((8, paths), f32))
    full = end_ref.shape[0]
    end_ref[width:full, :] = jnp.zeros((full - width, paths), f32)
    value = 1.0 / (2.0 + 0.4 * jnp.sum(norm, axis=0, keepdims=True) / width)
    first = jnp.where(level == 0.0, value, 0.0)
    remaining = horizon - start_t * step_len
    coef = share / remaining
    hot = start_hot(start_t, steps_k)
    rows_ref[...] = jnp.concatenate(
        [level, start_t, first, share, coef, jnp.zeros((3, paths), f32)], axis=0
    )
    half = other_ref.shape[1]
    begin = (1 - my_side()) * half
    weighted_sums(end_ref, begin, other_ref, hot, coef * first, share * first, width, split3)


def own_sums_kernel(width, steps_k, end_ref, rows_ref, mine_ref, high_ref, mid_ref):
    _, start_t, first, share, coef = (rows_ref[r : r + 1, :] for r in range(5))
    hot = start_hot(start_t, steps_k)
    remaining = horizon - start_t * (horizon / steps_k)
    for c in range(0, end_ref.shape[0], LANES):
        y = end_ref[c : c + LANES, :]
        if c + LANES > width:
            row = lax.broadcasted_iota(i32, y.shape, 0) + (c - width)
            y = jnp.where((row >= 0) & (row < VALUE_COPIES), remaining, y)
        high_ref[c : c + LANES, :], mid_ref[c : c + LANES, :] = split2(y)
    begin = my_side() * mine_ref.shape[1]
    weighted_sums(end_ref, begin, mine_ref, hot, coef * first, share * first, width, split3)


def dots_over(z_half, buf, begin, end):
    steps_k, paths = buf.shape[0], buf.shape[2]
    later = lax.broadcasted_iota(i32, (steps_k, LANES), 0)
    total = jnp.zeros((steps_k, paths), f32)
    for i in range(steps_k - 1):
        open_rows = (later > i).astype(f32).astype(bf16)
        z_open = [
            z_half[:, c : c + LANES] * open_rows for c in range(0, z_half.shape[1], LANES)
        ]
        z_open = jnp.concatenate(z_open, axis=1)[:, : end - begin]
        total = total + dot(z_open, buf[i, begin:end, :])
    return total


def half_dots(z_half, side, buf, total_ref):
    width, half = buf.shape[1], z_half.shape[1]
    for which, begin, end in ((0, 0, min(half, width)), (1, half, width)):

        @pl.when(side == which)
        def _(begin=begin, end=end):
            total_ref[...] = dots_over(z_half, buf, begin, end)


def own_half_kernel(buf, z_ref, total_ref):
    half_dots(z_ref[...], my_side(), buf, total_ref)


def second_kernel(
    n_tm, buf, mine_ref, other_ref, total_ref, high_ref, mid_ref, rows_ref, *refs
):
    *out_refs, z_ref, part_ref, rest_ref = refs
    steps_k, width, paths = buf.shape
    step_len = horizon / steps_k
    half = mine_ref.shape[1]
    group = steps_k // n_tm
    side = my_side()
    half_dots(other_ref[...], 1 - side, buf, rest_ref)
    z_ref[side] = mine_ref[...].astype(f32)
    z_ref[1 - side] = other_ref[...].astype(f32)
    value_one = sum(
        z_ref[1, :, width + r - half : width + r - half + 1] for r in range(VALUE_COPIES)
    )
    level, start_t, first, share, coef = (rows_ref[r : r + 1, :] for r in range(5))
    at = lax.broadcasted_iota(i32, (steps_k, paths), 0)

    total = total_ref[...] + rest_ref[...]
    estimate = value_one + jnp.sqrt(jnp.float32(step_len)) * total
    drift = estimate - estimate * estimate * estimate
    lvl = level.astype(i32)
    fine = lax.shift_left(jnp.ones_like(lvl), LEVELS - 1 - lvl)
    on_fine = (at & (fine - 1)) == 0
    on_coarse = ((at & (2 * fine - 1)) == 0) & (lvl > 0)
    weight = jnp.where(on_fine, fine, 0) - jnp.where(on_coarse, 2 * fine, 0)
    weight = jnp.where(at.astype(f32) >= start_t, weight.astype(f32), 0.0) * step_len
    second = first + jnp.sum(weight * drift, axis=0, keepdims=True)
    hot = start_hot(start_t, steps_k)

    weights = jnp.concatenate(split3(hot.astype(f32) * (coef * second)), axis=0)
    for c in range(0, part_ref.shape[1], LANES):
        sums = sum(contract_last(weights, ref[c : c + LANES, :]) for ref in (high_ref, mid_ref))
        part_ref[:, c : c + LANES] = sum(
            sums[r : r + steps_k] for r in range(0, 3 * steps_k, steps_k)
        )
    me = lax.axis_index("tm")
    for away, out_ref in enumerate(out_refs):
        out_ref[...] = part_ref[pl.ds(pl.multiple_of((me ^ away) * group, group), group), :]


def last_kernel(width, *refs):
    *parts, value_ref, grad_ref, value_buf, grad_buf, sems = refs
    total = pairwise([part[...] for part in parts])
    group = total.shape[0]
    grad_buf[...] = total[:, :width]
    square = (group, group)
    eye = lax.broadcasted_iota(i32, square, 0) == lax.broadcasted_iota(i32, square, 1)
    column = jnp.broadcast_to(total[:, width : width + 1], square)
    value_buf[...] = jnp.sum(jnp.where(eye, column, 0.0), axis=0, keepdims=True)
    copies = [
        pltpu.make_async_copy(grad_buf, grad_ref, sems.at[0]),
        pltpu.make_async_copy(value_buf, value_ref, sems.at[1]),
    ]
    for copy in copies:
        copy.start()
    for copy in copies:
        copy.wait()


def params():
    return pltpu.CompilerParams(vmem_limit_bytes=VMEM_LIMIT)


def in_hbm(x):
    return pltpu.with_memory_space_constraint(x, pltpu.HBM)


def swap(x, flips, odd_flips=None):
    n_path, n_tm = lax.axis_size("path"), lax.axis_size("tm")
    even, odd = (path * n_tm + tm for path, tm in (flips, odd_flips or flips))
    pairs = [
        (i, i ^ (odd if side_of(i // n_tm, i % n_tm, n_path) else even))
        for i in range(lax.axis_size(("path", "tm")))
    ]
    return lax.ppermute(x, ("path", "tm"), pairs)


def parity(n):
    return bin(n).count("1") % 2


def side_of(path, tm, n_path):
    bits = tm
    for bit in range(n_path.bit_length() - 1):
        bits = bits + (path >> bit)
    return bits & 1


def my_side():
    return side_of(lax.axis_index("path"), lax.axis_index("tm"), lax.axis_size("path"))


def add_kernel(*refs):
    *parts, out_ref = refs
    out_ref[...] = pairwise([part[...] for part in parts])


def round_kernel(width, *refs):
    *parts, out_ref = refs
    total = pairwise([part[...] for part in parts])
    first = my_side() * total.shape[1] - width
    column = lax.broadcasted_iota(i32, total.shape, 1) + first
    high, middle, low = (part.astype(f32) for part in split3(total))
    out_ref[...] = jnp.where(column == 1, middle, jnp.where(column == 2, low, high)).astype(bf16)


def pairwise(parts):
    while len(parts) > 1:
        parts = [a + b for a, b in zip(parts[::2], parts[1::2])]
    return parts[0]


def local(kernel, dtype, parts):
    vmem = pl.BlockSpec(memory_space=pltpu.VMEM)
    return pl.pallas_call(
        kernel,
        out_shape=jax.ShapeDtypeStruct(parts[0].shape, dtype),
        in_specs=[vmem] * len(parts),
        out_specs=vmem,
        compiler_params=pltpu.CompilerParams(vmem_limit_bytes=SMALL_LIMIT),
    )(*parts)


def path_steps(n_path):
    steps, bit = [], 2
    while bit < n_path:
        steps.append((bit, 2 * bit, 3 * bit) if 2 * bit < n_path else (bit,))
        bit *= 4
    return steps


def tm_steps(n_tm):
    steps = [tuple(flip // 2 for flip in step) for step in path_steps(2 * n_tm)]
    return [(step[0], *step[:0:-1]) for step in steps]


def shards(n_path, n_tm, increments, level_table, time_table):
    paths, steps_k, width = increments.shape
    group = steps_k // n_tm
    full = round_up(width + VALUE_COPIES, 2 * LANES)
    half = full // 2
    inc = jnp.transpose(increments, (1, 2, 0))
    vmem = pl.BlockSpec(memory_space=pltpu.VMEM)
    hbm = pl.BlockSpec(memory_space=pltpu.HBM)
    chunks = width // chunk_rows(width)

    other, end, rows, held = pl.pallas_call(
        functools.partial(first_kernel, n_path, n_tm),
        out_shape=(
            jax.ShapeDtypeStruct((steps_k, half), f32),
            jax.ShapeDtypeStruct((full, paths), f32),
            jax.ShapeDtypeStruct((8, paths), f32),
            jax.ShapeDtypeStruct(inc.shape, bf16),
        ),
        in_specs=[hbm, hbm, hbm],
        out_specs=(vmem,) * 4,
        scratch_shapes=[
            pltpu.VMEM((1, level_table.shape[0]), i32),
            pltpu.VMEM((1, time_table.shape[0]), i32),
            pltpu.VMEM((steps_k, PACKED, paths), bf16),
            pltpu.SemaphoreType.DMA((chunks,)),
            pltpu.SemaphoreType.DMA((2,)),
        ],
        compiler_params=params(),
        name="first_iterate",
    )(inc, *(in_hbm(table.reshape(1, -1)) for table in (level_table, time_table)))

    other = swap(other, (1, 0))
    mine, high, mid = pl.pallas_call(
        functools.partial(own_sums_kernel, width, steps_k),
        out_shape=(
            jax.ShapeDtypeStruct((steps_k, half), f32),
            jax.ShapeDtypeStruct((full, paths), bf16),
            jax.ShapeDtypeStruct((full, paths), bf16),
        ),
        in_specs=[vmem] * 2,
        out_specs=(vmem,) * 3,
        compiler_params=pltpu.CompilerParams(vmem_limit_bytes=SMALL_LIMIT),
        cost_estimate=pl.CostEstimate(
            flops=6 * steps_k * half * paths, bytes_accessed=0, transcendentals=0
        ),
        name="own_sums",
    )(end, rows)
    parts = [mine, other]
    over_path = [[(flip + parity(flip), 0) for flip in step] for step in path_steps(n_path)]
    over_tm = [[(flip % 2, flip) for flip in step] for step in tm_steps(n_tm)]
    odd, even = over_tm + over_path, over_path + over_tm
    if [len(step) for step in even] != [len(step) for step in odd]:
        odd = even
    for even_step, odd_step in zip(even, odd):
        total = local(add_kernel, f32, parts)
        parts = [total] + [swap(total, *flips) for flips in zip(even_step, odd_step)]
    own = local(functools.partial(round_kernel, width), bf16, parts)

    other = swap(own, (1, 0))
    total = pl.pallas_call(
        own_half_kernel,
        out_shape=jax.ShapeDtypeStruct((steps_k, paths), f32),
        in_specs=[vmem] * 2,
        out_specs=vmem,
        compiler_params=params(),
        cost_estimate=pl.CostEstimate(
            flops=paths * steps_k * steps_k * width, bytes_accessed=0, transcendentals=0
        ),
        name="own_half",
    )(held, own)
    parts = pl.pallas_call(
        functools.partial(second_kernel, n_tm),
        out_shape=(jax.ShapeDtypeStruct((group, full), f32),) * n_tm,
        in_specs=[vmem] * 7,
        out_specs=(vmem,) * n_tm,
        scratch_shapes=[
            pltpu.VMEM((2, steps_k, half), f32),
            pltpu.VMEM((steps_k, full), f32),
            pltpu.VMEM((steps_k, paths), f32),
        ],
        compiler_params=params(),
        name="second_iterate",
    )(held, own, other, total, high, mid, rows)

    order = [away for away in (*range(2, n_tm), 1) if away < n_tm]
    own = pairwise([parts[0]] + [swap(parts[away], (1, away)) for away in order])
    parts = [own, swap(own, (1, 0))]
    for step in path_steps(n_path):
        total = pairwise(parts)
        parts = [total] + [swap(total, (flip + 1, 0)) for flip in step]
    value, grad = pl.pallas_call(
        functools.partial(last_kernel, width),
        out_shape=(
            jax.ShapeDtypeStruct((1, group), f32),
            jax.ShapeDtypeStruct((group, width), f32),
        ),
        in_specs=[vmem] * len(parts),
        out_specs=(hbm, hbm),
        scratch_shapes=[
            pltpu.VMEM((1, group), f32),
            pltpu.VMEM((group, width), f32),
            pltpu.SemaphoreType.DMA((2,)),
        ],
        compiler_params=pltpu.CompilerParams(vmem_limit_bytes=SMALL_LIMIT),
        name="last_sum",
    )(*parts)
    return value.reshape(group), grad


def solution(mesh):
    placed = (P(("path", "tm"), None, None), P(), P())
    return jax.shard_map(
        functools.partial(shards, mesh.shape["path"], mesh.shape["tm"]),
        mesh=mesh,
        in_specs=placed,
        out_specs=(P("tm"), P("tm", None)),
        check_vma=False,
    )
```
